128 devices in a mesh: dp: 32 (over x, z, core), mp: 4 (over y).
Axes of the slice: x: 4, y: 4, z: 4, core: 2. Of those that a mesh axis runs over, the one named last changes fastest.
Arguments:
- query_rows: bfloat16 [2048, 2560], P('dp', 'mp'), may hold values from -48 to 48
- doc_rows: bfloat16 [2048, 2560], P('dp', 'mp'), may hold values from -48 to 48
- head: bfloat16 [2560, 2560], P(None, 'mp'), may hold values from -0.125 to 0.125
- logit_scale: float32 [7], replicated, may hold values from 1 to 3
- loss_grad: float32 [2048, 7], P('dp'), may hold values from 0.5 to 2
- shortlist: int32 [2048, 128], P('dp'), may hold values from 0 to 127, as said below
- send_rows: int32 [32, 128], P('dp'), may hold values from -1 to 63, as said below
Outputs:
- query_grad: bfloat16 [2048, 2560], P('dp', 'mp')
- doc_grad: bfloat16 [2048, 2560], P('dp', 'mp')
- head_grad: float32 [2560, 2560], P('dp', 'mp')
The draws below stay inside these ranges and needn't reach their ends.
Inputs may be any that keep to these rules, and one draw needn't show every extreme that they name: shortlist[i, n] is a slot o * 4 + j of the rows fetched for the owner of query i, and send_rows at place j of the block owner o sends to that owner is never -1. send_rows[o, r * 4 + j] is a row among owner o's 64 documents, sent to owner r at place j; in each block of 4 places the rows are distinct and come first, -1 fills the rest; the block an owner sends to itself is always full.
All inputs are finite; a program needn't handle non-finite values.
Results may differ from the reference program's by a relative error of at most 0.014.
The reference program's roundings to bfloat16 on the way count: a program that leaves them out, or rounds other values in their place, can miss the bound.
Values may be sent and summed in bfloat16 or wider, within the bound.
A program may use at most 64 MiB of HBM per device.

```python
import math
import jax
import jax.numpy as jnp
from jax import lax

D = 2560
QL = 64
NEG = 128
NW = 7
NQ = 2048
FETCH_ROWS = 128
N_DP = 32


def fetch_plan(key):
    fetch_block = FETCH_ROWS // N_DP
    base_key = jax.random.fold_in(key, 7001)
    count_key, order_key, owner_key, pick_key = jax.random.split(base_key, 4)
    least_count = (fetch_block + 1) // 2
    counts = jax.random.randint(count_key, (N_DP, N_DP), least_count, fetch_block + 1)
    diagonal = jnp.arange(N_DP)[:, None] == jnp.arange(N_DP)[None, :]
    counts = jnp.where(diagonal, fetch_block, counts)
    ranking = jax.random.randint(order_key, (N_DP, N_DP, QL), 0, 1 << 20) * QL + jnp.arange(QL)[None, None, :]
    row_order = jnp.argsort(ranking, axis=2)[:, :, :fetch_block]
    place_ids = jnp.arange(fetch_block)[None, None, :]
    sent_rows = jnp.where(place_ids < counts[:, :, None], row_order, -1).astype(jnp.int32)
    send_rows = sent_rows.reshape(N_DP, N_DP * fetch_block)
    owners = jax.random.randint(owner_key, (NQ, NEG), 0, N_DP)
    requester = jnp.broadcast_to((jnp.arange(NQ) // QL)[:, None], (NQ, NEG))
    available = counts[owners, requester]
    place_pick = jax.random.randint(pick_key, (NQ, NEG), 0, 1 << 16) % available
    shortlist = (owners * fetch_block + place_pick).astype(jnp.int32)
    return (send_rows, shortlist)


def embed_pair(key):
    base_key = jax.random.fold_in(key, 7002)
    query_key, doc_key = jax.random.split(base_key, 2)
    query_vals = jax.random.normal(query_key, (NQ, D), jnp.float32)
    doc_vals = jax.random.normal(doc_key, (NQ, D), jnp.float32)
    return (query_vals, doc_vals)


def draw_query_rows(key, part):
    return embed_pair(key)[0].astype(jnp.bfloat16)


def draw_doc_rows(key, part):
    return embed_pair(key)[1].astype(jnp.bfloat16)


def draw_shortlist(key, part):
    return fetch_plan(key)[1]


def draw_send_rows(key, part):
    return fetch_plan(key)[0]


def block_levels(own_key, shape, cuts, least, high):
    def one(position, blocks):
        draws = jax.random.uniform(jax.random.fold_in(jax.random.fold_in(own_key, 6), position), (blocks,), jnp.float32, least / len(cuts), high / len(cuts))
        return jnp.repeat(jnp.exp(draws), shape[position] // blocks).reshape((-1,) + (1,) * (len(shape) - position - 1))

    level = one(*cuts[0])
    for cut in cuts[1:]:
        level = level * one(*cut)
    return level


def bell_draw(rng, extent, width, limit, cuts=(), kind=jnp.bfloat16):
    values = width * jax.random.normal(rng, extent, jnp.float32)
    if cuts:
        values = values * block_levels(rng, extent, cuts, -0.22, 0.18)
    return jnp.clip(values, -limit, limit).astype(kind)


def setup_inputs(seed: int = 0) -> dict:
    streams_of = jax.random.split(jax.random.key(seed), 8)
    return {
        "query_rows": draw_query_rows(jax.random.fold_in(streams_of[7], 71), 0),
        "doc_rows": draw_doc_rows(jax.random.fold_in(streams_of[7], 71), 0),
        "head": bell_draw(streams_of[2], (D, D), D ** -0.5, 0.125, ((1, 4),)),
        "logit_scale": jnp.clip(jnp.exp(jax.random.uniform(streams_of[3], (NW,), jnp.float32, math.log(1.0), math.log(3.0))), 1.0, 3.0),
        "loss_grad": jnp.clip(jnp.exp(math.log(2.0) - 1.3862944 * jax.random.uniform(streams_of[4], (NQ, NW), jnp.float32) ** block_levels(streams_of[4], (NQ, NW), ((0, 32),), -0.2, 0.2)), 0.5, 2.0),
        "shortlist": draw_shortlist(jax.random.fold_in(streams_of[7], 71), 0),
        "send_rows": draw_send_rows(jax.random.fold_in(streams_of[7], 71), 0),
    }


def width_bounds():
    return [0] + [D // 2 ** (NW - 1 - width_level) for width_level in range(NW)]

def softmax_terms(neg_score, pos_score, width_scale, loss_weight):
    neg_logit = neg_score * width_scale[:, None, None]
    pos_logit = pos_score * width_scale[:, None]
    highest = jnp.maximum(lax.optimization_barrier(jnp.max(neg_logit, axis=2)), pos_logit)
    neg_exp = jnp.exp(neg_logit - highest[:, :, None])
    pos_exp = jnp.exp(pos_logit - highest)
    denominator = lax.optimization_barrier(jnp.sum(neg_exp, axis=2)) + pos_exp
    row_weight = loss_weight * width_scale[:, None]
    neg_grad = neg_exp * (row_weight / denominator)[:, :, None]
    pos_grad = row_weight * (pos_exp / denominator - 1.0)
    return (neg_grad, pos_grad)

def suffix_sum(values):
    return jnp.flip(jnp.cumsum(jnp.flip(values, 0), axis=0), 0)

def reference(query_rows, doc_rows, head, logit_scale, loss_grad, shortlist, send_rows):
    bounds = width_bounds()
    fetch_block = FETCH_ROWS // N_DP
    query_proj = jnp.dot(query_rows, head, preferred_element_type=jnp.float32).astype(jnp.bfloat16)
    doc_proj = jnp.dot(doc_rows, head, preferred_element_type=jnp.float32).astype(jnp.bfloat16)
    widths = jnp.array(bounds[1:], jnp.float32)
    width_scale = logit_scale / jnp.sqrt(widths)
    slot_ids = jnp.arange(FETCH_ROWS, dtype=jnp.int32)
    slot_owner = slot_ids // fetch_block
    slot_place = slot_ids % fetch_block
    col_ids = jnp.arange(D, dtype=jnp.int32)
    seg_onehot = jnp.stack([((col_ids >= bounds[segment]) & (col_ids < bounds[segment + 1])).astype(jnp.float32) for segment in range(NW)])
    query_ids = jnp.arange(QL, dtype=jnp.int32)

    def one_owner(doc_accum, inputs):
        owner_index, owner_query, owner_doc, shortlisted, weight_rows = inputs
        local_rows = send_rows[slot_owner, owner_index * fetch_block + slot_place]
        is_valid = local_rows >= 0
        doc_ids = (slot_owner * QL + jnp.maximum(local_rows, 0)).astype(jnp.int32)
        fetched = doc_proj[doc_ids]
        pieces = []
        for segment in range(NW):
            lower, upper = (bounds[segment], bounds[segment + 1])
            pieces.append(jnp.dot(owner_query[:, lower:upper], fetched[:, lower:upper].T, preferred_element_type=jnp.float32))
        scores = jnp.cumsum(jnp.stack(pieces), axis=0)
        neg_score = jnp.take_along_axis(scores, jnp.broadcast_to(shortlisted[None], (NW, QL, NEG)), axis=2)
        pos_prod = owner_query.astype(jnp.float32) * owner_doc.astype(jnp.float32)
        pos_score = jnp.cumsum(jnp.dot(seg_onehot, pos_prod.T, precision=lax.Precision.HIGHEST), axis=0)
        neg_grad, pos_grad = softmax_terms(neg_score, pos_score, width_scale, weight_rows.T)
        seg_neg = suffix_sum(neg_grad)
        seg_pos = suffix_sum(pos_grad)
        coeff_dense = jax.vmap(lambda values: jnp.zeros((QL, FETCH_ROWS), jnp.float32).at[query_ids[:, None], shortlisted].add(values))(seg_neg).astype(jnp.bfloat16)
        pos_cols = jnp.dot(seg_pos.T, seg_onehot, precision=lax.Precision.HIGHEST)
        query_parts = []
        fetched_parts = []
        for segment in range(NW):
            lower, upper = (bounds[segment], bounds[segment + 1])
            query_parts.append(jnp.dot(coeff_dense[segment], fetched[:, lower:upper], preferred_element_type=jnp.float32))
            fetched_parts.append(jnp.dot(coeff_dense[segment].T, owner_query[:, lower:upper], preferred_element_type=jnp.float32))
        query_back = jnp.concatenate(query_parts, axis=1) + pos_cols * owner_doc.astype(jnp.float32)
        fetched_grad = jnp.concatenate(fetched_parts, axis=1)
        targets = jnp.where(is_valid, doc_ids, NQ).astype(jnp.int32)
        doc_accum = doc_accum.at[targets].add(fetched_grad, mode='drop')
        own_start = (owner_index * QL).astype(jnp.int32)
        own_rows = lax.dynamic_slice_in_dim(doc_accum, own_start, QL, 0) + pos_cols * owner_query.astype(jnp.float32)
        doc_accum = lax.dynamic_update_slice_in_dim(doc_accum, own_rows, own_start, 0)
        return (doc_accum, query_back.astype(jnp.bfloat16))
    owner_range = jnp.arange(N_DP, dtype=jnp.int32)
    inputs = (owner_range, query_proj.reshape(N_DP, QL, D), doc_proj.reshape(N_DP, QL, D), shortlist.reshape(N_DP, QL, NEG), loss_grad.reshape(N_DP, QL, NW))
    doc_accum, query_back = lax.scan(one_owner, jnp.zeros((NQ, D), jnp.float32), inputs)
    grad_proj_q = query_back.reshape(NQ, D)
    grad_proj_d = doc_accum.astype(jnp.bfloat16)
    query_grad = jnp.dot(grad_proj_q, head.T, preferred_element_type=jnp.float32).astype(jnp.bfloat16)
    doc_grad = jnp.dot(grad_proj_d, head.T, preferred_element_type=jnp.float32).astype(jnp.bfloat16)
    head_grad = jnp.dot(query_rows.T, grad_proj_q, preferred_element_type=jnp.float32) + jnp.dot(doc_rows.T, grad_proj_d, preferred_element_type=jnp.float32)
    return (query_grad, doc_grad, head_grad)
```

```python
import functools
import math

import jax
import jax.numpy as jnp
from jax import lax
from jax.experimental import pallas as pl
from jax.experimental.pallas import tpu as pltpu
from jax.sharding import PartitionSpec as P

NW = 7
LOCAL = 5
MESH = pl.DeviceIdType.MESH
F32 = jnp.float32
BF16 = jnp.bfloat16


def remote(src, dst, send_sem, recv_sem, device):
    return pltpu.make_async_remote_copy(
        src_ref=src,
        dst_ref=dst,
        send_sem=send_sem,
        recv_sem=recv_sem,
        device_id=device,
        device_id_type=MESH,
    )


def contract(a, b, da, db):
    return lax.dot_general(a, b, (((da,), (db,)), ((), ())), preferred_element_type=F32)


def softmax_terms(score, pos, count, scale, weight):
    logit = jnp.where(count > 0.0, score * scale, -jnp.inf)
    pos_logit = pos * scale
    highest = jnp.maximum(jnp.max(logit, axis=1, keepdims=True), pos_logit)
    neg_exp = count * jnp.exp(logit - highest)
    pos_exp = jnp.exp(pos_logit - highest)
    denominator = jnp.sum(neg_exp, axis=1, keepdims=True) + pos_exp
    row_weight = weight * scale
    return neg_exp * (row_weight / denominator), row_weight * (pos_exp / denominator - 1.0)


def kernel(
    scale_ref, loss_ref, short_ref, send_ref, q_hbm, d_hbm, head_hbm,
    qg_ref, dg_ref, hg_ref,
    rows, head, rows_t, rt_buf, grads,
    out_buf, fetched, back_buf, returned,
    score_buf, part_q, got_q, part_d, got_d, part_h, got_h,
    load_sem, ag_s, ag_r, fe_s, fe_r, sc_s, sc_r, rt_s, rt_r, ba_s, ba_r,
    gq_s, gq_r, gd_s, gd_r, pq_s, pq_r, pd_s, pd_r, hg_s, hg_r,
):
    n_dp, n_mp, ql, cols = 32, 4, 64, 640
    group = 8
    slots = 128
    block = 4
    hrows = 80
    me = lax.axis_index("dp")
    my = lax.axis_index("mp")
    x = me // group
    g = me % group
    feature_total = n_mp * cols
    bounds = [0] + [feature_total // 2 ** (NW - 1 - w) for w in range(NW)]

    def row_block(m):
        return pl.ds(pl.multiple_of(m * cols, cols), cols)

    load_q = pltpu.make_async_copy(q_hbm, rows.at[my, pl.ds(0, ql)], load_sem.at[0])
    load_d = pltpu.make_async_copy(d_hbm, rows.at[my, pl.ds(ql, ql)], load_sem.at[1])
    load_q.start()
    load_d.start()
    order = (0, 1, 3, 2)
    load_h = []
    for k in order:
        src = (my + n_mp - k) % n_mp
        copy = pltpu.make_async_copy(
            head_hbm.at[row_block(src)], head.at[row_block(src)], load_sem.at[2 + k]
        )
        copy.start()
        load_h.append(copy)

    barrier = pltpu.get_barrier_semaphore()
    for k in range(1, n_mp):
        pl.semaphore_signal(
            barrier, inc=1, device_id=(me, (my + k) % n_mp), device_id_type=MESH
        )

    def greet(k, carry):
        pl.semaphore_signal(
            barrier, inc=1, device_id=((me + k) % n_dp, my), device_id_type=MESH
        )
        return carry

    lax.fori_loop(1, n_dp, greet, 0)

    short = short_ref[...]
    lane = lax.broadcasted_iota(jnp.int32, (ql, slots), 1)

    def count_step(j, carry):
        held, total = carry
        for k in range(8):
            now = held if k == 0 else pltpu.roll(held, k, 1)
            total = total + jnp.where(now == lane, 1.0, 0.0)
        return pltpu.roll(held, 8, 1), total

    _, count = lax.fori_loop(0, slots // 8, count_step, (short, jnp.zeros((ql, slots), F32)))
    pick = jnp.where(
        lax.broadcasted_iota(jnp.int32, (ql, slots), 0) == send_ref[...], 1.0, 0.0
    ).astype(BF16)

    load_q.wait()
    load_d.wait()
    pl.semaphore_wait(barrier, n_mp - 1 + n_dp - 1)

    sends = []
    for k in (1, 3, 2):
        copy = remote(
            rows.at[my], rows.at[my], ag_s.at[k], ag_r.at[k], (me, (my + k) % n_mp)
        )
        copy.start()
        sends.append(copy)
    acc = None
    for j, k in enumerate(order):
        src = (my + n_mp - k) % n_mp
        load_h[j].wait()
        if k:
            remote(rows.at[my], rows.at[src], ag_s.at[k], ag_r.at[k], (me, my)).wait_recv()
        term = jnp.dot(rows[src], head[row_block(src), :], preferred_element_type=F32)
        acc = term if acc is None else acc + term
    qp = acc[:ql].astype(BF16)
    dp = acc[ql:].astype(BF16)

    picked = contract(pick, dp, 0, 0).astype(BF16)
    out_buf[...] = picked.reshape(n_dp, block, cols)

    def fetch_send(k, carry):
        peer = (me + k) % n_dp
        remote(out_buf.at[peer], fetched.at[me], fe_s.at[k], fe_r.at[k], (peer, my)).start()
        return carry

    lax.fori_loop(1, n_dp, fetch_send, 0)
    fetched[me] = out_buf[me]

    for m in range(n_mp):
        rows_t[m] = rows[m].T
    for k in range(1, group):
        peer = (g + k) % group
        at = pl.multiple_of(peer * hrows, 16)
        to = pl.multiple_of(g * slots, slots)
        copy = remote(
            rows_t.at[:, pl.ds(at, hrows), :],
            rt_buf.at[:, :, pl.ds(to, slots)],
            rt_s.at[k],
            rt_r.at[k],
            (x * group + peer, my),
        )
        copy.start()
        sends.append(copy)
    rt_buf[:, :, pl.ds(pl.multiple_of(g * slots, slots), slots)] = rows_t[
        :, pl.ds(pl.multiple_of(g * hrows, 16), hrows), :
    ]

    col = lax.broadcasted_iota(jnp.int32, (1, cols), 1)
    seg_col = [
        jnp.where((col >= bounds[s]) & (col < bounds[s + 1]), 1.0, 0.0) for s in range(LOCAL)
    ]
    q_seg = jnp.concatenate([qp * m.astype(BF16) for m in seg_col], axis=0)
    product = qp.astype(F32) * dp.astype(F32)
    pos_prefix = [
        jnp.sum(
            product * jnp.where(col < bounds[s + 1], 1.0, 0.0), axis=1, keepdims=True
        )
        for s in range(LOCAL)
    ]

    def fetch_wait(k, carry):
        src = (me + n_dp - k) % n_dp
        remote(out_buf.at[me], fetched.at[src], fe_s.at[k], fe_r.at[k], (me, my)).wait_recv()
        return carry

    lax.fori_loop(1, n_dp, fetch_wait, 0)
    docs = fetched[...].reshape(slots, cols)
    pieces = contract(q_seg, docs, 1, 1)
    scores = []
    for s in range(LOCAL):
        piece = pieces[s * ql : (s + 1) * ql]
        scores.append(piece if s == 0 else scores[-1] + piece)

    diag = lax.broadcasted_iota(jnp.int32, (ql, slots), 0) == lane
    pos_row = jnp.sum(
        jnp.where(diag, jnp.broadcast_to(pos_prefix[-1], (ql, slots)), 0.0), axis=0, keepdims=True
    )
    score_buf[my, 0:ql, :] = scores[-1]
    score_buf[my, ql : ql + 8, :] = jnp.broadcast_to(pos_row, (8, slots))
    for k in (2, 1, 3):
        copy = remote(
            score_buf.at[my], score_buf.at[my], sc_s.at[k], sc_r.at[k], (me, (my + k) % n_mp)
        )
        copy.start()
        sends.append(copy)

    weight = loss_ref[...]

    def width(w, score, pos):
        scale = scale_ref[w] * (1.0 / math.sqrt(bounds[w + 1]))
        return softmax_terms(score, pos, count, scale, weight[:, w : w + 1])

    narrow = [width(w, scores[w], pos_prefix[w]) for w in range(LOCAL)]
    doc_seg = [docs * m.astype(BF16) for m in seg_col]
    doc_seg = jnp.concatenate(doc_seg, axis=0)

    for k in (1, 3, 2):
        src = (my + n_mp - k) % n_mp
        remote(score_buf.at[my], score_buf.at[src], sc_s.at[k], sc_r.at[k], (me, my)).wait_recv()
    parts = [score_buf[m, 0:ql, :] for m in range(n_mp)]
    pos_parts = [
        jnp.sum(
            jnp.where(diag, jnp.concatenate([score_buf[m, ql : ql + 8, :]] * 8, axis=0), 0.0),
            axis=1,
            keepdims=True,
        )
        for m in range(n_mp)
    ]
    score5, pos5 = parts[0] + parts[1], pos_parts[0] + pos_parts[1]
    neg5, posg5 = width(5, score5, pos5)
    neg6, posg6 = width(6, score5 + (parts[2] + parts[3]), pos5 + (pos_parts[2] + pos_parts[3]))
    run_neg = neg6 + jnp.where(my <= 1, neg5, 0.0)
    run_pos = posg6 + jnp.where(my <= 1, posg5, 0.0)
    coeff = [None] * LOCAL
    pos_cols = jnp.zeros((ql, cols), F32)
    for s in reversed(range(LOCAL)):
        run_neg = run_neg + jnp.where(my == 0, narrow[s][0], 0.0)
        run_pos = run_pos + jnp.where(my == 0, narrow[s][1], 0.0)
        coeff[s] = run_neg.astype(BF16)
        pos_cols = pos_cols + run_pos * seg_col[s]

    by_slot = contract(jnp.concatenate(coeff, axis=0), q_seg, 0, 0).astype(BF16)
    back_buf[...] = by_slot.reshape(n_dp, block, cols)

    def back_send(k, carry):
        peer = (me + k) % n_dp
        remote(back_buf.at[peer], returned.at[me], ba_s.at[k], ba_r.at[k], (peer, my)).start()
        return carry

    lax.fori_loop(1, n_dp, back_send, 0)
    returned[me] = back_buf[me]

    query_back = jnp.dot(jnp.concatenate(coeff, axis=1), doc_seg, preferred_element_type=F32)
    grad_q = (query_back + pos_cols * dp.astype(F32)).astype(BF16)

    partner = x * group + (g + 1 - 2 * (g % 2))

    def spread(first, send_sem, recv_sem, grad):
        at = pl.ds(pl.multiple_of(g * slots + first, ql), ql)
        grads[at, :] = grad
        for k in (4, 2, 6):
            peer = x * group + (g + k) % group
            copy = remote(grads.at[at], grads.at[at], send_sem.at[k], recv_sem.at[k], (peer, my))
            copy.start()
            sends.append(copy)
        copy = remote(grads.at[at], grads.at[at], send_sem.at[0], recv_sem.at[0], (partner, my))
        copy.start()
        sends.append(copy)

    def forward(first, send_sem, recv_sem):
        for k in (2, 6, 4):
            src = (g + group - k) % group
            at = pl.ds(pl.multiple_of(src * slots + first, ql), ql)
            remote(grads.at[at], grads.at[at], send_sem.at[k], recv_sem.at[k], (me, my)).wait_recv()
            copy = remote(
                grads.at[at], grads.at[at], send_sem.at[k + 1], recv_sem.at[k + 1], (partner, my)
            )
            copy.start()
            sends.append(copy)

    def settle(first, send_sem, recv_sem):
        other = g + 1 - 2 * (g % 2)
        for k in (0, 2, 6, 4):
            src = (other + group - k) % group
            at = pl.ds(pl.multiple_of(src * slots + first, ql), ql)
            slot = 0 if k == 0 else k + 1
            remote(
                grads.at[at], grads.at[at], send_sem.at[slot], recv_sem.at[slot], (me, my)
            ).wait_recv()

    def share(grad, part, got, send_sem, recv_sem):
        for k in (2, 1, 3):
            peer = (my + k) % n_mp
            part[k] = contract(grad, head[row_block(peer), :], 1, 1).astype(BF16)
            copy = remote(part.at[k], got.at[k], send_sem.at[k], recv_sem.at[k], (me, peer))
            copy.start()
            sends.append(copy)
        return contract(grad, head[row_block(my), :], 1, 1)

    def gather_parts(own, part, got, send_sem, recv_sem):
        for k in (1, 3, 2):
            remote(part.at[k], got.at[k], send_sem.at[k], recv_sem.at[k], (me, my)).wait_recv()
            own = own + got[k].astype(F32)
        return own

    spread(0, gq_s, gq_r, grad_q)
    own_q = share(grad_q, part_q, got_q, pq_s, pq_r)

    def back_wait(k, carry):
        src = (me + n_dp - k) % n_dp
        remote(back_buf.at[me], returned.at[src], ba_s.at[k], ba_r.at[k], (me, my)).wait_recv()
        return carry

    lax.fori_loop(1, n_dp, back_wait, 0)
    doc_back = jnp.dot(pick, returned[...].reshape(slots, cols), preferred_element_type=F32)
    grad_d = (pos_cols * qp.astype(F32) + doc_back).astype(BF16)
    spread(ql, gd_s, gd_r, grad_d)
    forward(0, gq_s, gq_r)
    own_d = share(grad_d, part_d, got_d, pd_s, pd_r)
    qg_ref[...] = gather_parts(own_q, part_q, got_q, pq_s, pq_r).astype(BF16)

    forward(ql, gd_s, gd_r)
    for k in range(1, group):
        src = (g + group - k) % group
        remote(
            rows_t.at[:, pl.ds(0, hrows), :],
            rt_buf.at[:, :, pl.ds(pl.multiple_of(src * slots, slots), slots)],
            rt_s.at[k],
            rt_r.at[k],
            (me, my),
        ).wait_recv()
    settle(0, gq_s, gq_r)
    settle(ql, gd_s, gd_r)
    everyone = grads[...]
    for k in (2, 1, 3):
        peer = (x + k) % n_mp
        part_h[k] = jnp.dot(rt_buf[peer], everyone, preferred_element_type=F32).astype(BF16)
        copy = remote(
            part_h.at[k], got_h.at[k], hg_s.at[k], hg_r.at[k], (peer * group + g, my)
        )
        copy.start()
        sends.append(copy)
    own_h = jnp.dot(rt_buf[x], everyone, preferred_element_type=F32)
    dg_ref[...] = gather_parts(own_d, part_d, got_d, pd_s, pd_r).astype(BF16)
    hg_ref[...] = gather_parts(own_h, part_h, got_h, hg_s, hg_r)

    def drain(k, carry):
        peer = (me + k) % n_dp
        remote(out_buf.at[peer], fetched.at[me], fe_s.at[k], fe_r.at[k], (peer, my)).wait_send()
        remote(back_buf.at[peer], returned.at[me], ba_s.at[k], ba_r.at[k], (peer, my)).wait_send()
        return carry

    lax.fori_loop(1, n_dp, drain, 0)
    for copy in sends:
        copy.wait_send()


def on_device(query_rows, doc_rows, head, logit_scale, loss_grad, shortlist, send_rows):
    ql, cols = query_rows.shape
    dma = pltpu.SemaphoreType.DMA
    vmem = pl.BlockSpec(memory_space=pltpu.VMEM)
    hbm = pl.BlockSpec(memory_space=pl.ANY)
    return pl.pallas_call(
        kernel,
        out_shape=(
            jax.ShapeDtypeStruct((ql, cols), BF16),
            jax.ShapeDtypeStruct((ql, cols), BF16),
            jax.ShapeDtypeStruct((80, cols), F32),
        ),
        in_specs=[pl.BlockSpec(memory_space=pltpu.SMEM), vmem, vmem, vmem, hbm, hbm, hbm],
        out_specs=(vmem, vmem, vmem),
        scratch_shapes=[
            pltpu.VMEM((4, 2 * ql, cols), BF16),
            pltpu.VMEM((4 * cols, cols), BF16),
            pltpu.VMEM((4, cols, 2 * ql), BF16),
            pltpu.VMEM((4, 80, 1024), BF16),
            pltpu.VMEM((1024, cols), BF16),
            pltpu.VMEM((32, 4, cols), BF16),
            pltpu.VMEM((32, 4, cols), BF16),
            pltpu.VMEM((32, 4, cols), BF16),
            pltpu.VMEM((32, 4, cols), BF16),
            pltpu.VMEM((4, ql + 8, 128), F32),
            pltpu.VMEM((4, ql, cols), BF16),
            pltpu.VMEM((4, ql, cols), BF16),
            pltpu.VMEM((4, ql, cols), BF16),
            pltpu.VMEM((4, ql, cols), BF16),
            pltpu.VMEM((4, 80, cols), BF16),
            pltpu.VMEM((4, 80, cols), BF16),
            dma((6,)), dma((4,)), dma((4,)), dma((32,)), dma((32,)), dma((4,)), dma((4,)),
            dma((8,)), dma((8,)), dma((32,)), dma((32,)),
            dma((8,)), dma((8,)), dma((8,)), dma((8,)),
            dma((4,)), dma((4,)), dma((4,)), dma((4,)), dma((4,)), dma((4,)),
        ],
        compiler_params=pltpu.CompilerParams(
            collective_id=0, has_side_effects=True, vmem_limit_bytes=48 * 1024 * 1024
        ),
    )(logit_scale, loss_grad, shortlist, send_rows, query_rows, doc_rows, head)


def solution(mesh):
    placed = (
        P("dp", "mp"),
        P("dp", "mp"),
        P(None, "mp"),
        P(),
        P("dp", None),
        P("dp", None),
        P("dp", None),
    )
    return jax.shard_map(
        on_device,
        mesh=mesh,
        in_specs=placed,
        out_specs=(P("dp", "mp"), P("dp", "mp"), P("dp", "mp")),
        check_vma=False,
    )
```

```python
import functools
import math

import jax
import jax.numpy as jnp
from jax import lax
from jax.experimental import pallas as pl
from jax.experimental.pallas import tpu as pltpu
from jax.sharding import PartitionSpec as P

NW = 7
LOCAL = 5
MESH = pl.DeviceIdType.MESH
F32 = jnp.float32
BF16 = jnp.bfloat16


def remote(src, dst, send_sem, recv_sem, device):
    return pltpu.make_async_remote_copy(
        src_ref=src,
        dst_ref=dst,
        send_sem=send_sem,
        recv_sem=recv_sem,
        device_id=device,
        device_id_type=MESH,
    )


class Phases:
    def __init__(self):
        self.open = None

    def __call__(self, name):
        if self.open is not None:
            self.open.__exit__(None, None, None)
        self.open = jax.named_scope(name) if name else None
        if self.open is not None:
            self.open.__enter__()


def contract(a, b, da, db):
    return lax.dot_general(a, b, (((da,), (db,)), ((), ())), preferred_element_type=F32)


def softmax_terms(score, pos, count, scale, weight):
    logit = jnp.where(count > 0.0, score * scale, -jnp.inf)
    pos_logit = pos * scale
    highest = jnp.maximum(jnp.max(logit, axis=1, keepdims=True), pos_logit)
    neg_exp = count * jnp.exp(logit - highest)
    pos_exp = jnp.exp(pos_logit - highest)
    denominator = jnp.sum(neg_exp, axis=1, keepdims=True) + pos_exp
    row_weight = weight * scale
    return neg_exp * (row_weight / denominator), row_weight * (pos_exp / denominator - 1.0)


def kernel(
    scale_hbm, loss_hbm, short_hbm, send_hbm, q_hbm, d_hbm, head_hbm,
    qg_ref, dg_ref, hg_ref,
    scale_ref, loss_ref, short_ref, send_ref, rows, head, rows_t, rt_buf, grads,
    out_buf, fetched, back_buf, returned,
    score_buf, part_q, got_q, part_d, got_d, part_h, got_h,
    load_sem, ag_s, ag_r, fe_s, fe_r, sc_s, sc_r, rt_s, rt_r, ba_s, ba_r,
    gq_s, gq_r, gd_s, gd_r, pq_s, pq_r, pd_s, pd_r, hg_s, hg_r,
):
    n_dp, n_mp, ql, cols = 32, 4, 64, 640
    group = 8
    slots = 128
    block = 4
    hrows = 80
    me = lax.axis_index("dp")
    my = lax.axis_index("mp")
    x = me // group
    g = me % group
    feature_total = n_mp * cols
    bounds = [0] + [feature_total // 2 ** (NW - 1 - w) for w in range(NW)]

    def row_block(m):
        return pl.ds(pl.multiple_of(m * cols, cols), cols)

    phase = Phases()
    phase("loads")
    load_q = pltpu.make_async_copy(q_hbm, rows.at[my, pl.ds(0, ql)], load_sem.at[0])
    load_d = pltpu.make_async_copy(d_hbm, rows.at[my, pl.ds(ql, ql)], load_sem.at[1])
    load_short = pltpu.make_async_copy(short_hbm, short_ref, load_sem.at[6])
    load_send = pltpu.make_async_copy(send_hbm, send_ref, load_sem.at[7])
    load_loss = pltpu.make_async_copy(loss_hbm, loss_ref, load_sem.at[8])
    load_scale = pltpu.make_async_copy(scale_hbm, scale_ref, load_sem.at[9])
    load_d.start()
    load_q.start()
    load_short.start()
    load_send.start()
    load_loss.start()
    load_scale.start()
    order = (0, 1, 3, 2)
    load_h = []
    for k in order:
        src = (my + n_mp - k) % n_mp
        copy = pltpu.make_async_copy(
            head_hbm.at[row_block(src)], head.at[row_block(src)], load_sem.at[2 + k]
        )
        copy.start()
        load_h.append(copy)

    phase("greet")
    barrier = pltpu.get_barrier_semaphore()
    for k in range(1, n_mp):
        pl.semaphore_signal(
            barrier, inc=1, device_id=(me, (my + k) % n_mp), device_id_type=MESH
        )

    for k in range(1, n_dp):
        pl.semaphore_signal(
            barrier, inc=1, device_id=((me + k) % n_dp, my), device_id_type=MESH
        )

    phase("pick_map")
    load_send.wait()
    pick = jnp.where(
        lax.broadcasted_iota(jnp.int32, (ql, slots), 0) == send_ref[...], 1.0, 0.0
    ).astype(BF16)

    load_loss.wait()
    load_scale.wait()
    weight = loss_ref[...].T
    phase("barrier")
    load_q.wait()
    load_d.wait()
    rows_t[...] = rows[my].T
    mine = pl.ds(pl.multiple_of(g * slots, slots), slots)
    rt_buf[my, :, mine] = rows_t[pl.ds(pl.multiple_of(g * hrows, 16), hrows), :]
    pl.semaphore_wait(barrier, n_mp - 1 + n_dp - 1)

    right, left = (my + 1) % n_mp, (my + n_mp - 1) % n_mp
    far = (my + 2) % n_mp
    half = ql // 2
    sends = []

    def row_copy(part, way, piece, src):
        second = (way == 1) if piece == 2 else (piece == 1)
        at = pl.ds((1 - part) * ql + (half if second else 0), half)
        slot = part * 6 + way * 3 + piece
        return remote(
            rows.at[src, at], rows.at[src, at], ag_s.at[slot], ag_r.at[slot],
            (me, right if way == 0 else left),
        )

    def rows_start(part):
        for way, piece in ((0, 0), (1, 1), (0, 1), (1, 0)):
            copy = row_copy(part, way, piece, my)
            copy.start()
            sends.append(copy)

    def rows_relay(part):
        for way, src in ((0, left), (1, right)):
            row_copy(part, way, way, src).wait_recv()
            copy = row_copy(part, way, 2, src)
            copy.start()
            sends.append(copy)

    def rows_rest(part):
        row_copy(part, 0, 1, left).wait_recv()
        yield left
        row_copy(part, 1, 0, right).wait_recv()
        yield right
        row_copy(part, 0, 2, far).wait_recv()
        row_copy(part, 1, 2, far).wait_recv()
        yield far

    def product_of(part, src):
        at = (1 - part) * ql
        return jnp.dot(
            rows[src, at : at + ql, :], head[row_block(src), :], preferred_element_type=F32
        )

    def turn_copy(way, piece, src):
        second = (way == 1) if piece == 2 else (piece == 1)
        at = pl.ds(512 if second else 0, 512)
        slot = 8 + way * 3 + piece
        return remote(
            rt_buf.at[src, :, at], rt_buf.at[src, :, at], rt_s.at[slot], rt_r.at[slot],
            (me, right if way == 0 else left),
        )

    def turn_start():
        for k in range(1, group):
            src = (g + group - k) % group
            remote(
                rows_t.at[pl.ds(0, hrows)],
                rt_buf.at[my, :, pl.ds(pl.multiple_of(src * slots, slots), slots)],
                rt_s.at[k],
                rt_r.at[k],
                (me, my),
            ).wait_recv()
        for way, piece in ((0, 0), (1, 1), (0, 1), (1, 0)):
            copy = turn_copy(way, piece, my)
            copy.start()
            sends.append(copy)

    def turn_relay():
        for way, src in ((0, left), (1, right)):
            turn_copy(way, way, src).wait_recv()
            copy = turn_copy(way, 2, src)
            copy.start()
            sends.append(copy)

    def turn_rest():
        turn_copy(0, 1, left).wait_recv()
        turn_copy(1, 0, right).wait_recv()
        turn_copy(0, 2, far).wait_recv()
        turn_copy(1, 2, far).wait_recv()

    phase("rows_d")
    rows_start(0)
    for k in range(1, group):
        peer = (g + k) % group
        copy = remote(
            rows_t.at[pl.ds(pl.multiple_of(peer * hrows, 16), hrows)],
            rt_buf.at[my, :, mine],
            rt_s.at[k],
            rt_r.at[k],
            (x * group + peer, my),
        )
        copy.start()
        sends.append(copy)
    load_h[0].wait()
    acc = product_of(0, my)
    rows_relay(0)
    rows_start(1)
    for copy in load_h[1:]:
        copy.wait()
    for src in rows_rest(0):
        acc = acc + product_of(0, src)
    phase("pick")
    dp = acc.astype(BF16)

    picked = contract(pick, dp, 0, 0).astype(BF16)
    out_buf[...] = picked.reshape(n_dp, block, cols)

    phase("fetch")
    def fetch_send(k, carry):
        peer = (me + k) % n_dp
        remote(out_buf.at[peer], fetched.at[me], fe_s.at[k], fe_r.at[k], (peer, my)).start()
        return carry

    lax.fori_loop(1, n_dp, fetch_send, 0)
    fetched[me] = out_buf[me]

    phase("relay_q")
    rows_relay(1)
    phase("count")
    load_short.wait()
    short = short_ref[...]
    lane = lax.broadcasted_iota(jnp.int32, (ql, slots), 1)

    count = jnp.zeros((ql, slots), F32)
    for k in range(slots):
        count = count + jnp.where((short if k == 0 else pltpu.roll(short, k, 1)) == lane, 1.0, 0.0)
    phase("rows_q")
    acc = product_of(1, my)
    for src in rows_rest(1):
        acc = acc + product_of(1, src)
    qp = acc.astype(BF16)

    phase("mask")
    col = lax.broadcasted_iota(jnp.int32, (1, cols), 1)
    seg_col = [
        jnp.where((col >= bounds[s]) & (col < bounds[s + 1]), 1.0, 0.0) for s in range(LOCAL)
    ]
    q_seg = jnp.concatenate([qp * m.astype(BF16) for m in seg_col], axis=0)
    product = qp.astype(F32) * dp.astype(F32)
    pos_prefix = [
        jnp.sum(
            product * jnp.where(col < bounds[s + 1], 1.0, 0.0), axis=1, keepdims=True
        )
        for s in range(LOCAL)
    ]

    phase("fetch_wait")
    def fetch_wait(k, carry):
        src = (me + n_dp - k) % n_dp
        remote(out_buf.at[me], fetched.at[src], fe_s.at[k], fe_r.at[k], (me, my)).wait_recv()
        return carry

    lax.fori_loop(1, n_dp, fetch_wait, 0)
    phase("score")
    docs = fetched[...].reshape(slots, cols)
    pieces = contract(q_seg, docs, 1, 1)
    scores = []
    for s in range(LOCAL):
        piece = pieces[s * ql : (s + 1) * ql]
        scores.append(piece if s == 0 else scores[-1] + piece)

    diag = lax.broadcasted_iota(jnp.int32, (ql, slots), 0) == lane
    pos_row = jnp.sum(
        jnp.where(diag, jnp.broadcast_to(pos_prefix[-1], (ql, slots)), 0.0), axis=0, keepdims=True
    )
    score_buf[my, 0:ql, :] = scores[-1]
    score_buf[my, ql : ql + 8, :] = jnp.broadcast_to(pos_row, (8, slots))
    for k in (2, 1, 3):
        copy = remote(
            score_buf.at[my], score_buf.at[my], sc_s.at[k], sc_r.at[k], (me, (my + k) % n_mp)
        )
        copy.start()
        sends.append(copy)

    phase("narrow")
    def width(w, score, pos):
        scale = scale_ref[w] * (1.0 / math.sqrt(bounds[w + 1]))
        return softmax_terms(score, pos, count, scale, weight[:, w : w + 1])

    narrow = [width(w, scores[w], pos_prefix[w]) for w in range(LOCAL)]
    doc_seg = [docs * m.astype(BF16) for m in seg_col]
    doc_seg = jnp.concatenate(doc_seg, axis=0)

    phase("score_wait")
    for k in (1, 3, 2):
        src = (my + n_mp - k) % n_mp
        remote(score_buf.at[my], score_buf.at[src], sc_s.at[k], sc_r.at[k], (me, my)).wait_recv()
    turn_start()
    phase("wide")
    parts = [score_buf[m, 0:ql, :] for m in range(n_mp)]
    pos_parts = [
        jnp.sum(
            jnp.where(diag, jnp.concatenate([score_buf[m, ql : ql + 8, :]] * 8, axis=0), 0.0),
            axis=1,
            keepdims=True,
        )
        for m in range(n_mp)
    ]
    score5, pos5 = parts[0] + parts[1], pos_parts[0] + pos_parts[1]
    neg5, posg5 = width(5, score5, pos5)
    neg6, posg6 = width(6, score5 + (parts[2] + parts[3]), pos5 + (pos_parts[2] + pos_parts[3]))
    run_neg = neg6 + jnp.where(my <= 1, neg5, 0.0)
    run_pos = posg6 + jnp.where(my <= 1, posg5, 0.0)
    coeff = [None] * LOCAL
    pos_cols = jnp.zeros((ql, cols), F32)
    for s in reversed(range(LOCAL)):
        run_neg = run_neg + jnp.where(my == 0, narrow[s][0], 0.0)
        run_pos = run_pos + jnp.where(my == 0, narrow[s][1], 0.0)
        coeff[s] = run_neg.astype(BF16)
        pos_cols = pos_cols + run_pos * seg_col[s]

    phase("by_slot")
    by_slot = contract(jnp.concatenate(coeff, axis=0), q_seg, 0, 0).astype(BF16)
    back_buf[...] = by_slot.reshape(n_dp, block, cols)

    def back_send(k, carry):
        peer = (me + k) % n_dp
        remote(back_buf.at[peer], returned.at[me], ba_s.at[k], ba_r.at[k], (peer, my)).start()
        return carry

    lax.fori_loop(1, n_dp, back_send, 0)
    returned[me] = back_buf[me]

    phase("grad_q")
    query_back = jnp.dot(jnp.concatenate(coeff, axis=1), doc_seg, preferred_element_type=F32)
    grad_q = (query_back + pos_cols * dp.astype(F32)).astype(BF16)

    partner = x * group + (g + 1 - 2 * (g % 2))

    def spread(first, send_sem, recv_sem, grad):
        at = pl.ds(pl.multiple_of(g * slots + first, ql), ql)
        grads[at, :] = grad
        for k in (4, 2, 6):
            peer = x * group + (g + k) % group
            copy = remote(grads.at[at], grads.at[at], send_sem.at[k], recv_sem.at[k], (peer, my))
            copy.start()
            sends.append(copy)
        copy = remote(grads.at[at], grads.at[at], send_sem.at[0], recv_sem.at[0], (partner, my))
        copy.start()
        sends.append(copy)

    def forward(first, send_sem, recv_sem):
        for k in (2, 6, 4):
            src = (g + group - k) % group
            at = pl.ds(pl.multiple_of(src * slots + first, ql), ql)
            remote(grads.at[at], grads.at[at], send_sem.at[k], recv_sem.at[k], (me, my)).wait_recv()
            copy = remote(
                grads.at[at], grads.at[at], send_sem.at[k + 1], recv_sem.at[k + 1], (partner, my)
            )
            copy.start()
            sends.append(copy)

    def settle(first, send_sem, recv_sem):
        other = g + 1 - 2 * (g % 2)
        for k in (0, 2, 6, 4):
            src = (other + group - k) % group
            at = pl.ds(pl.multiple_of(src * slots + first, ql), ql)
            slot = 0 if k == 0 else k + 1
            remote(
                grads.at[at], grads.at[at], send_sem.at[slot], recv_sem.at[slot], (me, my)
            ).wait_recv()

    def share(grad, part, got, send_sem, recv_sem):
        for k in (2, 1, 3):
            peer = (my + k) % n_mp
            part[k] = contract(grad, head[row_block(peer), :], 1, 1).astype(BF16)
            copy = remote(part.at[k], got.at[k], send_sem.at[k], recv_sem.at[k], (me, peer))
            copy.start()
            sends.append(copy)
        return contract(grad, head[row_block(my), :], 1, 1)

    def gather_parts(own, part, got, send_sem, recv_sem):
        for k in (1, 3, 2):
            remote(part.at[k], got.at[k], send_sem.at[k], recv_sem.at[k], (me, my)).wait_recv()
            own = own + got[k].astype(F32)
        return own

    phase("spread_q")
    spread(0, gq_s, gq_r, grad_q)
    phase("turn_relay")
    turn_relay()
    phase("share_q")
    own_q = share(grad_q, part_q, got_q, pq_s, pq_r)

    phase("back_wait")
    def back_wait(k, carry):
        src = (me + n_dp - k) % n_dp
        remote(back_buf.at[me], returned.at[src], ba_s.at[k], ba_r.at[k], (me, my)).wait_recv()
        return carry

    lax.fori_loop(1, n_dp, back_wait, 0)
    phase("grad_d")
    doc_back = jnp.dot(pick, returned[...].reshape(slots, cols), preferred_element_type=F32)
    grad_d = (pos_cols * qp.astype(F32) + doc_back).astype(BF16)
    spread(ql, gd_s, gd_r, grad_d)
    phase("forward_q")
    forward(0, gq_s, gq_r)
    phase("share_d")
    own_d = share(grad_d, part_d, got_d, pd_s, pd_r)
    phase("query_out")
    qg_ref[...] = gather_parts(own_q, part_q, got_q, pq_s, pq_r).astype(BF16)

    phase("forward_d")
    forward(ql, gd_s, gd_r)
    phase("rt_wait")
    turn_rest()
    phase("settle")
    settle(0, gq_s, gq_r)
    settle(ql, gd_s, gd_r)
    phase("head")
    everyone = grads[...]
    for k in (2, 1, 3):
        peer = (x + k) % n_mp
        part_h[k] = jnp.dot(rt_buf[peer], everyone, preferred_element_type=F32).astype(BF16)
        copy = remote(
            part_h.at[k], got_h.at[k], hg_s.at[k], hg_r.at[k], (peer * group + g, my)
        )
        copy.start()
        sends.append(copy)
    own_h = jnp.dot(rt_buf[x], everyone, preferred_element_type=F32)
    phase("doc_out")
    dg_ref[...] = gather_parts(own_d, part_d, got_d, pd_s, pd_r).astype(BF16)
    phase("head_out")
    hg_ref[...] = gather_parts(own_h, part_h, got_h, hg_s, hg_r)

    phase("drain")
    def drain(k, carry):
        peer = (me + k) % n_dp
        remote(out_buf.at[peer], fetched.at[me], fe_s.at[k], fe_r.at[k], (peer, my)).wait_send()
        remote(back_buf.at[peer], returned.at[me], ba_s.at[k], ba_r.at[k], (peer, my)).wait_send()
        return carry

    lax.fori_loop(1, n_dp, drain, 0)
    for copy in sends:
        copy.wait_send()
    phase(None)


def on_device(query_rows, doc_rows, head, logit_scale, loss_grad, shortlist, send_rows):
    ql, cols = query_rows.shape
    dma = pltpu.SemaphoreType.DMA
    vmem = pl.BlockSpec(memory_space=pltpu.VMEM)
    hbm = pl.BlockSpec(memory_space=pltpu.HBM)
    operands = (logit_scale, loss_grad.T, shortlist, send_rows, query_rows, doc_rows, head)
    return pl.pallas_call(
        kernel,
        out_shape=(
            jax.ShapeDtypeStruct((ql, cols), BF16),
            jax.ShapeDtypeStruct((ql, cols), BF16),
            jax.ShapeDtypeStruct((80, cols), F32),
        ),
        in_specs=[hbm] * 7,
        out_specs=(vmem, vmem, vmem),
        scratch_shapes=[
            pltpu.SMEM((NW,), F32),
            pltpu.VMEM((NW, ql), F32),
            pltpu.VMEM((ql, 128), jnp.int32),
            pltpu.VMEM((1, 128), jnp.int32),
            pltpu.VMEM((4, 2 * ql, cols), BF16),
            pltpu.VMEM((4 * cols, cols), BF16),
            pltpu.VMEM((cols, 2 * ql), BF16),
            pltpu.VMEM((4, 80, 1024), BF16),
            pltpu.VMEM((1024, cols), BF16),
            pltpu.VMEM((32, 4, cols), BF16),
            pltpu.VMEM((32, 4, cols), BF16),
            pltpu.VMEM((32, 4, cols), BF16),
            pltpu.VMEM((32, 4, cols), BF16),
            pltpu.VMEM((4, ql + 8, 128), F32),
            pltpu.VMEM((4, ql, cols), BF16),
            pltpu.VMEM((4, ql, cols), BF16),
            pltpu.VMEM((4, ql, cols), BF16),
            pltpu.VMEM((4, ql, cols), BF16),
            pltpu.VMEM((4, 80, cols), BF16),
            pltpu.VMEM((4, 80, cols), BF16),
            dma((10,)), dma((12,)), dma((12,)), dma((32,)), dma((32,)), dma((4,)), dma((4,)),
            dma((14,)), dma((14,)), dma((32,)), dma((32,)),
            dma((8,)), dma((8,)), dma((8,)), dma((8,)),
            dma((4,)), dma((4,)), dma((4,)), dma((4,)), dma((4,)), dma((4,)),
        ],
        compiler_params=pltpu.CompilerParams(
            collective_id=0, has_side_effects=True, vmem_limit_bytes=48 * 1024 * 1024
        ),
    )(*[pltpu.with_memory_space_constraint(a, pltpu.HBM) for a in operands])


def solution(mesh):
    placed = (
        P("dp", "mp"),
        P("dp", "mp"),
        P(None, "mp"),
        P(),
        P("dp", None),
        P("dp", None),
        P("dp", None),
    )
    return jax.shard_map(
        on_device,
        mesh=mesh,
        in_specs=placed,
        out_specs=(P("dp", "mp"), P("dp", "mp"), P("dp", "mp")),
        check_vma=False,
    )
```

```python
import functools
import math

import jax
import jax.numpy as jnp
from jax import lax
from jax.experimental import pallas as pl
from jax.experimental.pallas import tpu as pltpu
from jax.sharding import PartitionSpec as P

NW = 7
LOCAL = 5
MESH = pl.DeviceIdType.MESH
F32 = jnp.float32
BF16 = jnp.bfloat16


def remote(src, dst, send_sem, recv_sem, device):
    return pltpu.make_async_remote_copy(
        src_ref=src,
        dst_ref=dst,
        send_sem=send_sem,
        recv_sem=recv_sem,
        device_id=device,
        device_id_type=MESH,
    )


class Phases:
    def __init__(self):
        self.open = None

    def __call__(self, name):
        if self.open is not None:
            self.open.__exit__(None, None, None)
        self.open = jax.named_scope(name) if name else None
        if self.open is not None:
            self.open.__enter__()


def contract(a, b, da, db):
    return lax.dot_general(a, b, (((da,), (db,)), ((), ())), preferred_element_type=F32)


def softmax_terms(score, pos, count, scale, weight):
    logit = jnp.where(count > 0.0, score * scale, -jnp.inf)
    pos_logit = pos * scale
    highest = jnp.maximum(jnp.max(logit, axis=1, keepdims=True), pos_logit)
    neg_exp = count * jnp.exp(logit - highest)
    pos_exp = jnp.exp(pos_logit - highest)
    denominator = jnp.sum(neg_exp, axis=1, keepdims=True) + pos_exp
    row_weight = weight * scale
    return neg_exp * (row_weight / denominator), row_weight * (pos_exp / denominator - 1.0)


def kernel(
    scale_hbm, loss_hbm, short_hbm, send_hbm, q_hbm, d_hbm, head_hbm,
    qg_hbm, dg_hbm, hg_hbm,
    qg_ref, dg_ref, hg_ref,
    scale_ref, loss_ref, short_ref, send_ref, rows, head, rows_t, rt_buf, grads,
    out_buf, fetched, back_buf, returned,
    score_buf, part_q, got_q, part_d, got_d, full_h, part_h, got_h,
    load_sem, ag_s, ag_r, fe_s, fe_r, sc_s, sc_r, rt_s, rt_r, ba_s, ba_r,
    gr_s, gr_r, gp_r, pq_s, pq_r, pd_s, pd_r, hg_s, hg_r, word,
):
    n_dp, n_mp, ql, cols = 32, 4, 64, 640
    group = 8
    slots = 128
    block = 4
    hrows = 40
    me = lax.axis_index("dp")
    my = lax.axis_index("mp")
    x = me // group
    g = me % group
    z = g // 2
    feature_total = n_mp * cols
    bounds = [0] + [feature_total // 2 ** (NW - 1 - w) for w in range(NW)]

    def row_block(m):
        return pl.ds(pl.multiple_of(m * cols, cols), cols)

    phase = Phases()
    phase("loads")
    load_q = pltpu.make_async_copy(q_hbm, rows.at[my, pl.ds(0, ql)], load_sem.at[0])
    load_d = pltpu.make_async_copy(d_hbm, rows.at[my, pl.ds(ql, ql)], load_sem.at[1])
    load_short = pltpu.make_async_copy(short_hbm, short_ref, load_sem.at[6])
    load_send = pltpu.make_async_copy(send_hbm, send_ref, load_sem.at[7])
    load_loss = pltpu.make_async_copy(loss_hbm, loss_ref, load_sem.at[8])
    load_scale = pltpu.make_async_copy(scale_hbm, scale_ref, load_sem.at[9])
    load_d.start()
    load_q.start()
    load_short.start()
    load_send.start()
    load_loss.start()
    load_scale.start()
    order = (0, 1, 3, 2)
    load_h = []
    for k in order:
        src = (my + n_mp - k) % n_mp
        copy = pltpu.make_async_copy(
            head_hbm.at[row_block(src)], head.at[row_block(src)], load_sem.at[2 + k]
        )
        copy.start()
        load_h.append(copy)

    phase("greet")
    right, left = (my + 1) % n_mp, (my + n_mp - 1) % n_mp
    far = (my + 2) % n_mp
    core = me % 2
    partner = me + 1 - 2 * core
    x_near = ((me + group) % n_dp, (me + n_dp - group) % n_dp)
    z_near = (x * group + (g + 2) % group, x * group + (g + 6) % group)
    barrier = pltpu.get_barrier_semaphore()
    near = [(me, right), (me, left), (me, far), (partner, my)]
    near += [(peer, my) for peer in x_near + z_near]
    for device in near:
        pl.semaphore_signal(barrier, inc=1, device_id=device, device_id_type=MESH)

    def await_sent(ref, sem):
        remote(ref, ref, sem, sem, (me, my)).wait_send()

    def await_got(ref, sem):
        remote(ref, ref, sem, sem, (me, my)).wait_recv()

    def tell(step, peers):
        for peer in peers:
            pl.semaphore_signal(
                word.at[step], inc=1, device_id=(peer, my), device_id_type=MESH
            )

    def hear(step, count):
        pl.semaphore_wait(word.at[step], count)

    load_d.wait()
    pl.semaphore_wait(barrier, len(near))

    half, quarter = ql // 2, ql // 4

    def row_copy(part, slot, src):
        first, count, peer = (
            (0, half, far),
            (0, ql, right),
            (half, quarter, left),
            (half + quarter, quarter, left),
            (0, half, left),
            (half, quarter, left),
            (half + quarter, quarter, left),
        )[slot]
        at = pl.ds((1 - part) * ql + first, count)
        slot = part * 7 + slot
        return remote(
            rows.at[src, at], rows.at[src, at], ag_s, ag_r.at[slot], (me, peer)
        )

    def rows_start(part):
        for slot in (0, 2, 1, 3, 4):
            row_copy(part, slot, my).start()

    def rows_relay(part):
        for slot in (2, 3):
            row_copy(part, slot, right).wait_recv()
            row_copy(part, slot + 3, right).start()

    def rows_right(part):
        row_copy(part, 4, right).wait_recv()
        return product_of(part, right)

    def rows_left(part):
        row_copy(part, 1, left).wait_recv()
        return product_of(part, left)

    def rows_far(part):
        for slot in (0, 5, 6):
            row_copy(part, slot, far).wait_recv()
        return product_of(part, far)

    def product_of(part, src):
        at = (1 - part) * ql
        return jnp.dot(
            rows[src, at : at + ql, :], head[row_block(src), :], preferred_element_type=F32
        )

    along = (
        (g, lambda j: x * group + j, lambda j: j * group + g, x),
        (x * 2 + core, lambda j: (j // 2) * group + z * 2 + j % 2,
         lambda j: x * group + j * 2 + core, z),
    )

    def turned(axis, j):
        if axis == 0:
            return rows_t.at[:, j // 2, j % 2, pl.ds(0, hrows), :]
        return rows_t.at[j // 2, :, j % 2, pl.ds(hrows, hrows), :]

    def turn_copy(axis, to, src):
        return remote(
            turned(axis, to),
            rt_buf.at[axis, :, :, pl.ds(pl.multiple_of(src * slots, slots), slots)],
            rt_s,
            rt_r,
            (along[axis][1](to), my),
        )

    def turn_start():
        for m in range(n_mp):
            rows_t[m] = rows[m].T.reshape(n_mp, 2, 2 * hrows, slots)
        for axis in range(2):
            own = along[axis][0]
            for k in range(1, group):
                turn_copy(axis, (own + k) % group, own).start()
            at = pl.ds(pl.multiple_of(own * slots, slots), slots)
            rt_buf[axis, :, :, at] = turned(axis, own)[...]

    rt_others = rt_buf.at[:, :, :, pl.ds(0, (group - 1) * slots)]

    phase("rows_d")
    rows_start(0)
    tell(0, x_near)
    load_h[0].wait()
    acc = product_of(0, my)
    load_send.wait()
    pick = jnp.where(
        lax.broadcasted_iota(jnp.int32, (ql, slots), 0) == send_ref[...], 1.0, 0.0
    ).astype(BF16)

    for copy in load_h[1:]:
        copy.wait()
    hear(0, 2)
    tell(1, z_near)
    phase("relay_d")
    rows_relay(0)
    load_q.wait()
    rows_start(1)
    hear(1, 2)
    tell(2, z_near)
    phase("right_d")
    acc = acc + rows_right(0)
    hear(2, 2)
    tell(3, (partner,))
    phase("left_d")
    acc = acc + rows_left(0)
    phase("far_d")
    acc = acc + rows_far(0)
    hear(3, 1)
    phase("pick")
    dp = acc.astype(BF16)

    picked = contract(pick, dp, 0, 0).astype(BF16)
    out_buf[...] = picked.reshape(n_dp, block, cols)

    phase("fetch")
    def fetch_send(k, carry):
        peer = (me + k) % n_dp
        remote(out_buf.at[peer], fetched.at[me], fe_s, fe_r, (peer, my)).start()
        return carry

    lax.fori_loop(1, n_dp, fetch_send, 0)
    fetched[me] = out_buf[me]

    phase("relay_q")
    rows_relay(1)
    phase("count")
    load_loss.wait()
    load_scale.wait()
    weight = loss_ref[...].T
    load_short.wait()
    short = short_ref[...]
    lane = lax.broadcasted_iota(jnp.int32, (ql, slots), 1)

    count = jnp.zeros((ql, slots), F32)
    for k in range(slots):
        count = count + jnp.where((short if k == 0 else pltpu.roll(short, k, 1)) == lane, 1.0, 0.0)
    phase("rows_q")
    acc = product_of(1, my) + rows_right(1) + rows_left(1) + rows_far(1)
    qp = acc.astype(BF16)

    phase("mask")
    col = lax.broadcasted_iota(jnp.int32, (1, cols), 1)
    seg_col = [
        jnp.where((col >= bounds[s]) & (col < bounds[s + 1]), 1.0, 0.0) for s in range(LOCAL)
    ]
    q_seg = jnp.concatenate([qp * m.astype(BF16) for m in seg_col], axis=0)
    product = qp.astype(F32) * dp.astype(F32)
    pos_prefix = [
        jnp.sum(
            product * jnp.where(col < bounds[s + 1], 1.0, 0.0), axis=1, keepdims=True
        )
        for s in range(LOCAL)
    ]

    phase("fetch_wait")
    await_got(fetched.at[pl.ds(0, n_dp - 1)], fe_r)
    phase("turn")
    turn_start()
    phase("score")
    docs = fetched[...].reshape(slots, cols)
    pieces = contract(q_seg, docs, 1, 1)
    scores = []
    for s in range(LOCAL):
        piece = pieces[s * ql : (s + 1) * ql]
        scores.append(piece if s == 0 else scores[-1] + piece)

    diag = lax.broadcasted_iota(jnp.int32, (ql, slots), 0) == lane
    pos_row = jnp.sum(
        jnp.where(diag, jnp.broadcast_to(pos_prefix[-1], (ql, slots)), 0.0), axis=0, keepdims=True
    )
    score_buf[my, 0:ql, :] = scores[-1]
    score_buf[my, ql : ql + 8, :] = jnp.broadcast_to(pos_row, (8, slots))
    for peer in (far, right, left):
        remote(score_buf.at[my], score_buf.at[my], sc_s, sc_r, (me, peer)).start()

    phase("narrow")
    def width(w, score, pos):
        scale = scale_ref[w] * (1.0 / math.sqrt(bounds[w + 1]))
        return softmax_terms(score, pos, count, scale, weight[:, w : w + 1])

    narrow = [width(w, scores[w], pos_prefix[w]) for w in range(LOCAL)]
    doc_seg = [docs * m.astype(BF16) for m in seg_col]
    wide_at = 256
    docs_low = jnp.concatenate([m[:, :wide_at] for m in doc_seg[:4]], axis=0)
    docs_high = jnp.concatenate([m[:, wide_at:] for m in doc_seg[3:]], axis=0)

    phase("score_wait")
    await_got(score_buf.at[pl.ds(0, n_mp - 1)], sc_r)
    phase("wide")
    parts = [score_buf[m, 0:ql, :] for m in range(n_mp)]
    pos_parts = [
        jnp.sum(
            jnp.where(diag, jnp.concatenate([score_buf[m, ql : ql + 8, :]] * 8, axis=0), 0.0),
            axis=1,
            keepdims=True,
        )
        for m in range(n_mp)
    ]
    score5, pos5 = parts[0] + parts[1], pos_parts[0] + pos_parts[1]
    neg5, posg5 = width(5, score5, pos5)
    neg6, posg6 = width(6, score5 + (parts[2] + parts[3]), pos5 + (pos_parts[2] + pos_parts[3]))
    run_neg = neg6 + jnp.where(my <= 1, neg5, 0.0)
    run_pos = posg6 + jnp.where(my <= 1, posg5, 0.0)
    coeff = [None] * LOCAL
    pos_cols = jnp.zeros((ql, cols), F32)
    for s in reversed(range(LOCAL)):
        run_neg = run_neg + jnp.where(my == 0, narrow[s][0], 0.0)
        run_pos = run_pos + jnp.where(my == 0, narrow[s][1], 0.0)
        coeff[s] = run_neg.astype(BF16)
        pos_cols = pos_cols + run_pos * seg_col[s]

    phase("by_slot")
    by_slot = jnp.concatenate(
        [
            contract(jnp.concatenate(coeff[:4], axis=0), q_seg[: 4 * ql, :wide_at], 0, 0),
            contract(jnp.concatenate(coeff[3:], axis=0), q_seg[3 * ql :, wide_at:], 0, 0),
        ],
        axis=1,
    ).astype(BF16)
    back_buf[...] = by_slot.reshape(n_dp, block, cols)

    def back_send(k, carry):
        peer = (me + k) % n_dp
        remote(back_buf.at[peer], returned.at[me], ba_s, ba_r, (peer, my)).start()
        return carry

    lax.fori_loop(1, n_dp, back_send, 0)
    returned[me] = back_buf[me]

    phase("grad_q")
    query_back = jnp.concatenate(
        [
            jnp.dot(jnp.concatenate(coeff[:4], axis=1), docs_low, preferred_element_type=F32),
            jnp.dot(jnp.concatenate(coeff[3:], axis=1), docs_high, preferred_element_type=F32),
        ],
        axis=1,
    )
    grad_q = (query_back + pos_cols * dp.astype(F32)).astype(BF16)

    def gr_at(axis, part, slot):
        if slot in (0, 3, 5, 7):
            return gp_r
        return gr_r.at[axis, slot - 8 if part == 0 else 5 + slot // 2]

    def grad_copy(axis, part, slot, src, peer, first=0, count=ql):
        at = pl.ds(pl.multiple_of(src * slots + part * ql + first, half), count)
        return remote(
            grads.at[axis, at], grads.at[axis, at],
            gr_s, gr_at(axis, part, slot), (peer, my),
        )

    def grad_send(*args):
        grad_copy(*args).start()

    def keep(part, grad):
        for axis in range(2):
            at = pl.ds(pl.multiple_of(along[axis][0] * slots + part * ql, ql), ql)
            grads[axis, at, :] = grad

    def spread_d(grad):
        keep(1, grad)
        for k in (4, 2, 6, 0):
            for axis in range(2):
                own, device, _, _ = along[axis]
                peer = partner if k == 0 else device((own + k) % group)
                grad_send(axis, 1, k, own, peer)

    def spread_q(grad):
        keep(0, grad)
        for axis in range(2):
            own, device, _, _ = along[axis]
            up, down = device((own + 2) % group), device((own + 6) % group)
            grad_send(axis, 0, 8, own, up, 0, half)
            grad_send(axis, 0, 9, own, down, half, half)
            grad_send(axis, 0, 10, own, up, half, half)
            grad_send(axis, 0, 11, own, down, 0, half)
            grad_send(axis, 0, 0, own, partner)

    def relay_q():
        for axis in range(2):
            own, device, _, _ = along[axis]
            up, down = (own + 2) % group, (own + 6) % group
            grad_copy(axis, 0, 8, down, me, 0, half).wait_recv()
            grad_send(axis, 0, 12, down, device(up), 0, half)
            grad_copy(axis, 0, 9, up, me, half, half).wait_recv()
            grad_send(axis, 0, 13, up, device(down), half, half)

    def forward_q():
        for axis in range(2):
            own = along[axis][0]
            up, down, beyond = (own + 2) % group, (own + 6) % group, (own + 4) % group
            grad_copy(axis, 0, 10, down, me, half, half).wait_recv()
            grad_send(axis, 0, 3, down, partner)
            grad_copy(axis, 0, 11, up, me, 0, half).wait_recv()
            grad_send(axis, 0, 7, up, partner)
        for axis in range(2):
            beyond = (along[axis][0] + 4) % group
            grad_copy(axis, 0, 12, beyond, me, 0, half).wait_recv()
            grad_copy(axis, 0, 13, beyond, me, half, half).wait_recv()
            grad_send(axis, 0, 5, beyond, partner)

    def forward_d():
        for k in (2, 6, 4):
            for axis in range(2):
                src = (along[axis][0] + group - k) % group
                grad_copy(axis, 1, k, src, me).wait_recv()
                grad_send(axis, 1, k + 1, src, partner)

    def share(grad, part, got, send_sem, recv_sem):
        for k in (2, 1, 3):
            peer = (my + k) % n_mp
            part[k] = contract(grad, head[row_block(peer), :], 1, 1).astype(BF16)
            remote(part.at[k], got.at[k], send_sem, recv_sem, (me, peer)).start()
        return contract(grad, head[row_block(my), :], 1, 1)

    def gather_parts(own, got):
        for k in (1, 3, 2):
            own = own + got[k].astype(F32)
        return own

    phase("spread_q")
    spread_q(grad_q)
    phase("share_q")
    own_q = share(grad_q, part_q, got_q, pq_s, pq_r)

    phase("relay_gq")
    relay_q()
    phase("back_wait")
    await_got(returned.at[pl.ds(0, n_dp - 1)], ba_r)
    phase("grad_d")
    doc_back = jnp.dot(pick, returned[...].reshape(slots, cols), preferred_element_type=F32)
    grad_d = (pos_cols * qp.astype(F32) + doc_back).astype(BF16)
    spread_d(grad_d)
    phase("share_d")
    own_d = share(grad_d, part_d, got_d, pd_s, pd_r)
    phase("forward_q")
    forward_q()
    phase("forward_d")
    forward_d()
    phase("rt_wait")
    await_got(rt_others, rt_r)
    phase("settle")
    await_got(grads.at[0], gp_r)
    phase("head")
    own_h = []
    for axis in range(2):
        mine = along[axis][3]
        total = jnp.dot(
            rt_buf[axis].reshape(n_mp * hrows, group * slots), grads[axis],
            preferred_element_type=F32,
        )
        full_h[axis] = total.reshape(n_mp, hrows, cols)
        part_h[axis] = full_h[axis].astype(BF16)
        for k in (2, 1, 3):
            peer = (mine + k) % n_mp
            remote(
                part_h.at[axis, peer], got_h.at[axis, k], hg_s, hg_r, (along[axis][2](peer), my)
            ).start()
        own_h.append(full_h[axis, mine])
    phase("query_out")
    await_got(got_q.at[pl.ds(1, n_mp - 1)], pq_r)
    qg_ref[...] = gather_parts(own_q, got_q).astype(BF16)

    save_q = pltpu.make_async_copy(qg_ref, qg_hbm, load_sem.at[10])
    save_q.start()
    phase("doc_out")
    await_got(got_d.at[pl.ds(1, n_mp - 1)], pd_r)
    dg_ref[...] = gather_parts(own_d, got_d).astype(BF16)
    save_d = pltpu.make_async_copy(dg_ref, dg_hbm, load_sem.at[11])
    save_d.start()
    phase("head_out")
    await_got(got_h.at[:, pl.ds(1, n_mp - 1)], hg_r)
    for axis in range(2):
        hg_ref[axis * hrows : (axis + 1) * hrows, :] = gather_parts(own_h[axis], got_h.at[axis])
    phase("drain")
    save_h = pltpu.make_async_copy(hg_ref, hg_hbm, load_sem.at[12])
    save_h.start()
    await_sent(rows.at[pl.ds(0, 3)], ag_s)
    await_sent(out_buf.at[pl.ds(0, n_dp - 1)], fe_s)
    await_sent(rt_others, rt_s)
    await_sent(score_buf.at[pl.ds(0, n_mp - 1)], sc_s)
    await_sent(back_buf.at[pl.ds(0, n_dp - 1)], ba_s)
    await_sent(grads.at[:, pl.ds(0, 896)], gr_s)
    await_sent(part_q.at[pl.ds(1, n_mp - 1)], pq_s)
    await_sent(part_d.at[pl.ds(1, n_mp - 1)], pd_s)
    await_sent(part_h.at[:, pl.ds(1, n_mp - 1)], hg_s)
    phase("saved")
    for copy in (save_q, save_d, save_h):
        copy.wait()
    phase(None)


def hand_out(a, b, c, out_a, out_b, out_c, sem):
    copies = [
        pltpu.make_async_copy(src, dst, sem.at[i])
        for i, (src, dst) in enumerate(((c, out_c), (a, out_a), (b, out_b)))
    ]
    for copy in copies:
        copy.start()
    for copy in copies:
        copy.wait()


def on_device(query_rows, doc_rows, head, logit_scale, loss_grad, shortlist, send_rows):
    ql, cols = query_rows.shape
    dma = pltpu.SemaphoreType.DMA
    one = dma(())
    hbm = pl.BlockSpec(memory_space=pltpu.HBM)
    operands = (logit_scale, loss_grad.T, shortlist, send_rows, query_rows, doc_rows, head)
    shapes = (
        jax.ShapeDtypeStruct((ql, cols), BF16),
        jax.ShapeDtypeStruct((ql, cols), BF16),
        jax.ShapeDtypeStruct((80, cols), F32),
    )
    results = pl.pallas_call(
        kernel,
        out_shape=shapes,
        in_specs=[hbm] * 7,
        out_specs=(hbm, hbm, hbm),
        scratch_shapes=[
            pltpu.VMEM((ql, cols), BF16),
            pltpu.VMEM((ql, cols), BF16),
            pltpu.VMEM((80, cols), F32),
            pltpu.SMEM((NW,), F32),
            pltpu.VMEM((NW, ql), F32),
            pltpu.VMEM((ql, 128), jnp.int32),
            pltpu.VMEM((1, 128), jnp.int32),
            pltpu.VMEM((4, 2 * ql, cols), BF16),
            pltpu.VMEM((4 * cols, cols), BF16),
            pltpu.VMEM((4, 4, 2, 80, 128), BF16),
            pltpu.VMEM((2, 4, 40, 1024), BF16),
            pltpu.VMEM((2, 1024, cols), BF16),
            pltpu.VMEM((32, 4, cols), BF16),
            pltpu.VMEM((32, 4, cols), BF16),
            pltpu.VMEM((32, 4, cols), BF16),
            pltpu.VMEM((32, 4, cols), BF16),
            pltpu.VMEM((4, ql + 8, 128), F32),
            pltpu.VMEM((4, ql, cols), BF16),
            pltpu.VMEM((4, ql, cols), BF16),
            pltpu.VMEM((4, ql, cols), BF16),
            pltpu.VMEM((4, ql, cols), BF16),
            pltpu.VMEM((2, 4, 40, cols), F32),
            pltpu.VMEM((2, 4, 40, cols), BF16),
            pltpu.VMEM((2, 4, 40, cols), BF16),
            dma((13,)), one, dma((14,)), one, one, one, one, one, one, one, one,
            one, dma((2, 9)), one, one, one, one, one, one, one,
            pltpu.SemaphoreType.REGULAR((4,)),
        ],
        compiler_params=pltpu.CompilerParams(
            collective_id=0, has_side_effects=True, vmem_limit_bytes=48 * 1024 * 1024
        ),
    )(*[pltpu.with_memory_space_constraint(a, pltpu.HBM) for a in operands])
    anywhere = pl.BlockSpec(memory_space=pl.ANY)
    return pl.pallas_call(
        hand_out,
        out_shape=shapes,
        in_specs=[anywhere] * 3,
        out_specs=(anywhere,) * 3,
        scratch_shapes=[dma((3,))],
        compiler_params=pltpu.CompilerParams(vmem_limit_bytes=1024 * 1024),
    )(*results)


def solution(mesh):
    placed = (
        P("dp", "mp"),
        P("dp", "mp"),
        P(None, "mp"),
        P(),
        P("dp", None),
        P("dp", None),
        P("dp", None),
    )
    return jax.shard_map(
        on_device,
        mesh=mesh,
        in_specs=placed,
        out_specs=(P("dp", "mp"), P("dp", "mp"), P("dp", "mp")),
        check_vma=False,
    )
```

```python
import functools
import math

import jax
import jax.numpy as jnp
from jax import lax
from jax.experimental import pallas as pl
from jax.experimental.pallas import tpu as pltpu
from jax.sharding import PartitionSpec as P

NW = 7
LOCAL = 5
MESH = pl.DeviceIdType.MESH
F32 = jnp.float32
BF16 = jnp.bfloat16


def remote(src, dst, send_sem, recv_sem, device):
    return pltpu.make_async_remote_copy(
        src_ref=src,
        dst_ref=dst,
        send_sem=send_sem,
        recv_sem=recv_sem,
        device_id=device,
        device_id_type=MESH,
    )


class Phases:
    def __init__(self):
        self.open = None

    def __call__(self, name):
        if self.open is not None:
            self.open.__exit__(None, None, None)
        self.open = jax.named_scope(name) if name else None
        if self.open is not None:
            self.open.__enter__()


def contract(a, b, da, db):
    return lax.dot_general(a, b, (((da,), (db,)), ((), ())), preferred_element_type=F32)


def softmax_terms(score, pos, count, scale, weight):
    logit = jnp.where(count > 0.0, score * scale, -jnp.inf)
    pos_logit = pos * scale
    highest = jnp.maximum(jnp.max(logit, axis=1, keepdims=True), pos_logit)
    neg_exp = count * jnp.exp(logit - highest)
    pos_exp = jnp.exp(pos_logit - highest)
    denominator = jnp.sum(neg_exp, axis=1, keepdims=True) + pos_exp
    row_weight = weight * scale
    return neg_exp * (row_weight / denominator), row_weight * (pos_exp / denominator - 1.0)


def kernel(
    scale_hbm, loss_hbm, short_hbm, send_hbm, q_hbm, d_hbm, head_hbm,
    qg_ref, dg_ref, hg_ref,
    scale_ref, loss_ref, short_ref, send_ref, rows, head, rows_t, rt_buf, grads_0, grads_1,
    out_buf, fetched, back_buf, returned,
    score_buf, part_q, got_q, part_d, got_d,
    full_0, full_1, part_0, part_1, got_0, got_1,
    load_sem, ag_s, ag_r, fe_s, fe_r, sc_s, sc_r, rt_s, rt_r, ba_s, ba_r,
    gr_s, gr_r, gp_r, pq_s, pq_r, pd_s, pd_r, hg_s, hg_r, word,
):
    n_dp, n_mp, ql, cols = 32, 4, 64, 640
    group = 8
    slots = 128
    block = 4
    hrows = 80
    cuts = (0, 384, cols)
    grads, full_h, part_h, got_h = (
        (grads_0, grads_1), (full_0, full_1), (part_0, part_1), (got_0, got_1)
    )
    me = lax.axis_index("dp")
    my = lax.axis_index("mp")
    x = me // group
    g = me % group
    z = g // 2
    feature_total = n_mp * cols
    bounds = [0] + [feature_total // 2 ** (NW - 1 - w) for w in range(NW)]

    def row_block(m):
        return pl.ds(pl.multiple_of(m * cols, cols), cols)

    phase = Phases()
    phase("loads")
    load_q = pltpu.make_async_copy(q_hbm, rows.at[my, pl.ds(0, ql)], load_sem.at[0])
    load_d = pltpu.make_async_copy(d_hbm, rows.at[my, pl.ds(ql, ql)], load_sem.at[1])
    load_short = pltpu.make_async_copy(short_hbm, short_ref, load_sem.at[6])
    load_send = pltpu.make_async_copy(send_hbm, send_ref, load_sem.at[7])
    load_loss = pltpu.make_async_copy(loss_hbm, loss_ref, load_sem.at[8])
    load_scale = pltpu.make_async_copy(scale_hbm, scale_ref, load_sem.at[9])
    load_d.start()
    load_q.start()
    load_short.start()
    load_send.start()
    load_loss.start()
    load_scale.start()
    order = (0, 1, 3, 2)
    load_h = []
    for k in order:
        src = (my + n_mp - k) % n_mp
        copy = pltpu.make_async_copy(
            head_hbm.at[row_block(src)], head.at[row_block(src)], load_sem.at[2 + k]
        )
        copy.start()
        load_h.append(copy)

    phase("greet")
    right, left = (my + 1) % n_mp, (my + n_mp - 1) % n_mp
    far = (my + 2) % n_mp
    core = me % 2
    partner = me + 1 - 2 * core
    x_near = ((me + group) % n_dp, (me + n_dp - group) % n_dp)
    z_near = (x * group + (g + 2) % group, x * group + (g + 6) % group)
    barrier = pltpu.get_barrier_semaphore()
    near = [(me, right), (me, left), (me, far), (partner, my)]
    near += [(peer, my) for peer in x_near + z_near]
    for device in near:
        pl.semaphore_signal(barrier, inc=1, device_id=device, device_id_type=MESH)

    def await_sent(ref, sem):
        remote(ref, ref, sem, sem, (me, my)).wait_send()

    def await_got(ref, sem):
        remote(ref, ref, sem, sem, (me, my)).wait_recv()

    steps = [(i, j, k) for i in (2, 1, 3, 0) for j in (2, 1, 3, 0) for k in (0, 1)]
    steps.sort(key=lambda d: -(min(d[0], 4 - d[0]) + min(d[1], 4 - d[1])))
    others = [
        ((x + i) % 4 * group + (z + j) % 4 * 2 + (core if k == 0 else 1 - core))
        for i, j, k in steps
        if (i, j, k) != (0, 0, 0)
    ]

    def tell(step, peers):
        for peer in peers:
            pl.semaphore_signal(
                word.at[step], inc=1, device_id=(peer, my), device_id_type=MESH
            )

    def hear(step, count):
        pl.semaphore_wait(word.at[step], count)

    load_d.wait()
    pl.semaphore_wait(barrier, len(near))

    half, quarter = ql // 2, ql // 4

    def row_copy(part, slot, src):
        first, count, peer = (
            (0, half, far),
            (0, ql, right),
            (half, quarter, left),
            (half + quarter, quarter, left),
            (0, half, left),
            (half, quarter, left),
            (half + quarter, quarter, left),
        )[slot]
        at = pl.ds((1 - part) * ql + first, count)
        slot = part * 7 + slot
        return remote(
            rows.at[src, at], rows.at[src, at], ag_s, ag_r.at[slot], (me, peer)
        )

    def rows_start(part):
        for slot in (0, 2, 1, 3, 4):
            row_copy(part, slot, my).start()

    def rows_relay(part):
        for slot in (2, 3):
            row_copy(part, slot, right).wait_recv()
            row_copy(part, slot + 3, right).start()

    def rows_right(part):
        row_copy(part, 4, right).wait_recv()
        return product_of(part, right)

    def rows_left(part):
        row_copy(part, 1, left).wait_recv()
        return product_of(part, left)

    def rows_far(part):
        for slot in (0, 5, 6):
            row_copy(part, slot, far).wait_recv()
        return product_of(part, far)

    def product_of(part, src):
        at = (1 - part) * ql
        return jnp.dot(
            rows[src, at : at + ql, :], head[row_block(src), :], preferred_element_type=F32
        )

    along = (
        (g, lambda j: x * group + j, lambda j: j * group + g, x),
        (x * 2 + core, lambda j: (j // 2) * group + z * 2 + j % 2,
         lambda j: x * group + j * 2 + core, z),
    )

    def turned(axis, j):
        if axis == 0:
            return rows_t.at[:, j // 2, j % 2]
        return rows_t.at[j // 2, :, j % 2]

    def turn_copy(axis, to, src):
        return remote(
            turned(axis, to),
            rt_buf.at[axis, :, :, pl.ds(pl.multiple_of(src * slots, slots), slots)],
            rt_s,
            rt_r,
            (along[axis][1](to), my),
        )

    def turn_rows():
        for m in range(n_mp):
            rows_t[m] = rows[m].T.reshape(n_mp, 2, hrows, slots)

    def turn_start(axes):
        for axis in axes:
            own = along[axis][0]
            for k in range(1, group):
                turn_copy(axis, (own + k) % group, own).start()
            at = pl.ds(pl.multiple_of(own * slots, slots), slots)
            rt_buf[axis, :, :, at] = turned(axis, own)[...]

    rt_others = rt_buf.at[:, :, :, pl.ds(0, (group - 1) * slots)]

    phase("rows_d")
    rows_start(0)
    tell(0, x_near)
    load_h[0].wait()
    acc = product_of(0, my)
    load_send.wait()
    pick = jnp.where(
        lax.broadcasted_iota(jnp.int32, (ql, slots), 0) == send_ref[...], 1.0, 0.0
    ).astype(BF16)

    for copy in load_h[1:]:
        copy.wait()
    hear(0, 2)
    tell(1, z_near)
    phase("relay_d")
    rows_relay(0)
    load_q.wait()
    rows_start(1)
    hear(1, 2)
    tell(2, z_near)
    phase("right_d")
    acc = acc + rows_right(0)
    hear(2, 2)
    tell(3, (partner,))
    phase("left_d")
    acc = acc + rows_left(0)
    phase("far_d")
    acc = acc + rows_far(0)
    hear(3, 1)
    phase("pick")
    dp = acc.astype(BF16)

    picked = contract(pick, dp, 0, 0).astype(BF16)
    out_buf[...] = picked.reshape(n_dp, block, cols)

    phase("fetch")
    for peer in others:
        remote(out_buf.at[peer], fetched.at[me], fe_s, fe_r, (peer, my)).start()
    fetched[me] = out_buf[me]

    phase("relay_q")
    rows_relay(1)
    phase("count")
    load_loss.wait()
    load_scale.wait()
    weight = loss_ref[...].T
    load_short.wait()
    short = short_ref[...]
    lane = lax.broadcasted_iota(jnp.int32, (ql, slots), 1)

    count = jnp.zeros((ql, slots), F32)
    for k in range(slots):
        count = count + jnp.where((short if k == 0 else pltpu.roll(short, k, 1)) == lane, 1.0, 0.0)
    phase("rows_q")
    acc = product_of(1, my) + rows_right(1) + rows_left(1) + rows_far(1)
    qp = acc.astype(BF16)

    phase("turn0")
    turn_rows()
    turn_start((0,))
    phase("mask")
    col = lax.broadcasted_iota(jnp.int32, (1, cols), 1)
    seg_col = [
        jnp.where((col >= bounds[s]) & (col < bounds[s + 1]), 1.0, 0.0) for s in range(LOCAL)
    ]
    q_seg = jnp.concatenate([qp * m.astype(BF16) for m in seg_col], axis=0)
    product = qp.astype(F32) * dp.astype(F32)
    pos_prefix = [
        jnp.sum(
            product * jnp.where(col < bounds[s + 1], 1.0, 0.0), axis=1, keepdims=True
        )
        for s in range(LOCAL)
    ]

    phase("fetch_wait")
    await_got(fetched.at[pl.ds(0, n_dp - 1)], fe_r)
    phase("turn")
    turn_start((1,))
    phase("score")
    docs = fetched[...].reshape(slots, cols)
    pieces = contract(q_seg, docs, 1, 1)
    scores = []
    for s in range(LOCAL):
        piece = pieces[s * ql : (s + 1) * ql]
        scores.append(piece if s == 0 else scores[-1] + piece)

    diag = lax.broadcasted_iota(jnp.int32, (ql, slots), 0) == lane
    pos_row = jnp.sum(
        jnp.where(diag, jnp.broadcast_to(pos_prefix[-1], (ql, slots)), 0.0), axis=0, keepdims=True
    )
    score_buf[my, 0:ql, :] = scores[-1]
    score_buf[my, ql : ql + 8, :] = jnp.broadcast_to(pos_row, (8, slots))
    for peer in (far, right, left):
        remote(score_buf.at[my], score_buf.at[my], sc_s, sc_r, (me, peer)).start()

    phase("narrow")
    def width(w, score, pos):
        scale = scale_ref[w] * (1.0 / math.sqrt(bounds[w + 1]))
        return softmax_terms(score, pos, count, scale, weight[:, w : w + 1])

    narrow = [width(w, scores[w], pos_prefix[w]) for w in range(LOCAL)]
    doc_seg = [docs * m.astype(BF16) for m in seg_col]
    wide_at = 256
    docs_low = jnp.concatenate([m[:, :wide_at] for m in doc_seg[:4]], axis=0)
    docs_high = jnp.concatenate([m[:, wide_at:] for m in doc_seg[3:]], axis=0)

    phase("score_wait")
    await_got(score_buf.at[pl.ds(0, n_mp - 1)], sc_r)
    phase("wide")
    parts = [score_buf[m, 0:ql, :] for m in range(n_mp)]
    pos_parts = [
        jnp.sum(
            jnp.where(diag, jnp.concatenate([score_buf[m, ql : ql + 8, :]] * 8, axis=0), 0.0),
            axis=1,
            keepdims=True,
        )
        for m in range(n_mp)
    ]
    score5, pos5 = parts[0] + parts[1], pos_parts[0] + pos_parts[1]
    neg5, posg5 = width(5, score5, pos5)
    neg6, posg6 = width(6, score5 + (parts[2] + parts[3]), pos5 + (pos_parts[2] + pos_parts[3]))
    run_neg = neg6 + jnp.where(my <= 1, neg5, 0.0)
    run_pos = posg6 + jnp.where(my <= 1, posg5, 0.0)
    coeff = [None] * LOCAL
    pos_cols = jnp.zeros((ql, cols), F32)
    for s in reversed(range(LOCAL)):
        run_neg = run_neg + jnp.where(my == 0, narrow[s][0], 0.0)
        run_pos = run_pos + jnp.where(my == 0, narrow[s][1], 0.0)
        coeff[s] = run_neg.astype(BF16)
        pos_cols = pos_cols + run_pos * seg_col[s]

    phase("by_slot")
    by_slot = jnp.concatenate(
        [
            contract(jnp.concatenate(coeff[:4], axis=0), q_seg[: 4 * ql, :wide_at], 0, 0),
            contract(jnp.concatenate(coeff[3:], axis=0), q_seg[3 * ql :, wide_at:], 0, 0),
        ],
        axis=1,
    ).astype(BF16)
    back_buf[...] = by_slot.reshape(n_dp, block, cols)

    for peer in others:
        remote(back_buf.at[peer], returned.at[me], ba_s, ba_r, (peer, my)).start()
    returned[me] = back_buf[me]

    phase("grad_q")
    query_back = jnp.concatenate(
        [
            jnp.dot(jnp.concatenate(coeff[:4], axis=1), docs_low, preferred_element_type=F32),
            jnp.dot(jnp.concatenate(coeff[3:], axis=1), docs_high, preferred_element_type=F32),
        ],
        axis=1,
    )
    grad_q = (query_back + pos_cols * dp.astype(F32)).astype(BF16)

    def gr_at(axis, part, slot):
        if slot in (0, 3, 5, 7):
            return gp_r.at[slot // 2]
        return gr_r.at[axis, part, slot // 2 - 1]

    def grad_copy(axis, part, slot, src, peer):
        at = pl.ds(pl.multiple_of(src * slots + part * ql, ql), ql)
        return remote(
            grads[axis].at[at], grads[axis].at[at],
            gr_s.at[axis], gr_at(axis, part, slot), (peer, my),
        )

    def grad_send(*args):
        grad_copy(*args).start()

    def keep(part, grad):
        for axis in range(2):
            at = pl.ds(pl.multiple_of(along[axis][0] * slots + part * ql, ql), ql)
            grads[axis][at, :] = grad[:, cuts[axis] : cuts[axis + 1]]

    def spread(part, grad):
        keep(part, grad)
        for k in (4, 2, 6, 0):
            for axis in range(2):
                own, device, _, _ = along[axis]
                grad_send(axis, part, k, own, partner if k == 0 else device((own + k) % group))

    def forward(part, k):
        for axis in range(2):
            src = (along[axis][0] + group - k) % group
            grad_copy(axis, part, k, src, me).wait_recv()
            grad_send(axis, part, k + 1, src, partner)

    def share(grad, part, got, send_sem, recv_sem):
        for k in (2, 1, 3):
            peer = (my + k) % n_mp
            part[k] = contract(grad, head[row_block(peer), :], 1, 1).astype(BF16)
            remote(part.at[k], got.at[k], send_sem, recv_sem, (me, peer)).start()
        return contract(grad, head[row_block(my), :], 1, 1)

    def gather_parts(own, got):
        for k in (1, 3, 2):
            own = own + got[k].astype(F32)
        return own

    phase("share_q")
    own_q = share(grad_q, part_q, got_q, pq_s, pq_r)

    phase("spread_q")
    spread(0, grad_q)
    phase("back_wait")
    await_got(returned.at[pl.ds(0, n_dp - 1)], ba_r)
    phase("grad_d")
    doc_back = jnp.dot(pick, returned[...].reshape(slots, cols), preferred_element_type=F32)
    grad_d = (pos_cols * qp.astype(F32) + doc_back).astype(BF16)
    spread(1, grad_d)
    phase("share_d")
    own_d = share(grad_d, part_d, got_d, pd_s, pd_r)
    phase("forward_q")
    for k in (2, 6, 4):
        forward(0, k)
    await_got(rt_others, rt_r)
    chips = (z, x)
    total_h = [None, None]

    def chip_product(axis, k):
        at = pl.ds(pl.multiple_of((chips[axis] + 4 - k // 2) % 4 * 2 * slots, slots), 2 * slots)
        term = jnp.dot(
            rt_buf[axis, :, :, at].reshape(n_mp * hrows, 2 * slots), grads[axis][at, :],
            preferred_element_type=F32,
        )
        return term if total_h[axis] is None else total_h[axis] + term

    def chip_arrived(k):
        await_got(rows.at[0], gp_r.at[(k + 1) // 2 if k else 0])

    phase("own_h")
    chip_arrived(0)
    for axis in range(2):
        total_h[axis] = chip_product(axis, 0)
    phase("forward_d")
    for k in (2, 6, 4):
        forward(1, k)
    for k in (2, 6):
        phase("near_h")
        chip_arrived(k)
        for axis in range(2):
            total_h[axis] = chip_product(axis, k)
    phase("settle")
    chip_arrived(4)
    phase("head")
    own_h = []
    for axis in range(2):
        mine = along[axis][3]
        full_h[axis][...] = chip_product(axis, 4).reshape(n_mp, hrows, -1)
        part_h[axis][...] = full_h[axis][...].astype(BF16)
        for k in (2, 1, 3):
            peer = (mine + k) % n_mp
            remote(
                part_h[axis].at[peer], got_h[axis].at[k], hg_s.at[axis], hg_r.at[axis],
                (along[axis][2](peer), my),
            ).start()
        own_h.append(full_h[axis][mine])
    phase("query_out")
    await_got(got_q.at[pl.ds(1, n_mp - 1)], pq_r)
    qg_ref[...] = gather_parts(own_q, got_q).astype(BF16)

    phase("doc_out")
    await_got(got_d.at[pl.ds(1, n_mp - 1)], pd_r)
    dg_ref[...] = gather_parts(own_d, got_d).astype(BF16)
    phase("head_out")
    for axis in range(2):
        await_got(got_h[axis].at[pl.ds(1, n_mp - 1)], hg_r.at[axis])
        hg_ref[:, cuts[axis] : cuts[axis + 1]] = gather_parts(own_h[axis], got_h[axis])
    phase("drain")
    await_sent(rows.at[pl.ds(0, 3)], ag_s)
    await_sent(out_buf.at[pl.ds(0, n_dp - 1)], fe_s)
    await_sent(rt_others, rt_s)
    await_sent(score_buf.at[pl.ds(0, n_mp - 1)], sc_s)
    await_sent(back_buf.at[pl.ds(0, n_dp - 1)], ba_s)
    for axis in range(2):
        await_sent(grads[axis].at[pl.ds(0, 896)], gr_s.at[axis])
        await_sent(part_h[axis].at[pl.ds(1, n_mp - 1)], hg_s.at[axis])
    await_sent(part_q.at[pl.ds(1, n_mp - 1)], pq_s)
    await_sent(part_d.at[pl.ds(1, n_mp - 1)], pd_s)
    phase(None)


def hand_out(a, b, c, out_a, out_b, out_c, sem):
    copies = [
        pltpu.make_async_copy(src, dst, sem.at[i])
        for i, (src, dst) in enumerate(((c, out_c), (a, out_a), (b, out_b)))
    ]
    for copy in copies:
        copy.start()
    for copy in copies:
        copy.wait()


def on_device(query_rows, doc_rows, head, logit_scale, loss_grad, shortlist, send_rows):
    ql, cols = query_rows.shape
    dma = pltpu.SemaphoreType.DMA
    one = dma(())
    hbm = pl.BlockSpec(memory_space=pltpu.HBM)
    vmem = pl.BlockSpec(memory_space=pltpu.VMEM)
    operands = (logit_scale, loss_grad.T, shortlist, send_rows, query_rows, doc_rows, head)
    shapes = (
        jax.ShapeDtypeStruct((ql, cols), BF16),
        jax.ShapeDtypeStruct((ql, cols), BF16),
        jax.ShapeDtypeStruct((80, cols), F32),
    )
    results = pl.pallas_call(
        kernel,
        out_shape=shapes,
        in_specs=[hbm] * 7,
        out_specs=(vmem, vmem, vmem),
        scratch_shapes=[
            pltpu.SMEM((NW,), F32),
            pltpu.VMEM((NW, ql), F32),
            pltpu.VMEM((ql, 128), jnp.int32),
            pltpu.VMEM((1, 128), jnp.int32),
            pltpu.VMEM((4, 2 * ql, cols), BF16),
            pltpu.VMEM((4 * cols, cols), BF16),
            pltpu.VMEM((4, 4, 2, 80, 128), BF16),
            pltpu.VMEM((2, 4, 80, 1024), BF16),
            pltpu.VMEM((1024, 384), BF16),
            pltpu.VMEM((1024, 256), BF16),
            pltpu.VMEM((32, 4, cols), BF16),
            pltpu.VMEM((32, 4, cols), BF16),
            pltpu.VMEM((32, 4, cols), BF16),
            pltpu.VMEM((32, 4, cols), BF16),
            pltpu.VMEM((4, ql + 8, 128), F32),
            pltpu.VMEM((4, ql, cols), BF16),
            pltpu.VMEM((4, ql, cols), BF16),
            pltpu.VMEM((4, ql, cols), BF16),
            pltpu.VMEM((4, ql, cols), BF16),
            pltpu.VMEM((4, 80, 384), F32),
            pltpu.VMEM((4, 80, 256), F32),
            pltpu.VMEM((4, 80, 384), BF16),
            pltpu.VMEM((4, 80, 256), BF16),
            pltpu.VMEM((4, 80, 384), BF16),
            pltpu.VMEM((4, 80, 256), BF16),
            dma((10,)), one, dma((14,)), one, one, one, one, one, one, one, one,
            dma((2,)), dma((2, 2, 3)), dma((4,)), one, one, one, one, dma((2,)), dma((2,)),
            pltpu.SemaphoreType.REGULAR((4,)),
        ],
        compiler_params=pltpu.CompilerParams(
            collective_id=0, has_side_effects=True, vmem_limit_bytes=48 * 1024 * 1024
        ),
    )(*[pltpu.with_memory_space_constraint(a, pltpu.HBM) for a in operands])
    anywhere = pl.BlockSpec(memory_space=pl.ANY)
    return pl.pallas_call(
        hand_out,
        out_shape=shapes,
        in_specs=[anywhere] * 3,
        out_specs=(anywhere,) * 3,
        scratch_shapes=[dma((3,))],
        compiler_params=pltpu.CompilerParams(vmem_limit_bytes=1024 * 1024),
    )(*results)


def solution(mesh):
    placed = (
        P("dp", "mp"),
        P("dp", "mp"),
        P(None, "mp"),
        P(),
        P("dp", None),
        P("dp", None),
        P("dp", None),
    )
    return jax.shard_map(
        on_device,
        mesh=mesh,
        in_specs=placed,
        out_specs=(P("dp", "mp"), P("dp", "mp"), P("dp", "mp")),
        check_vma=False,
    )
```

```python
import functools
import math

import jax
import jax.numpy as jnp
from jax import lax
from jax.experimental import pallas as pl
from jax.experimental.pallas import tpu as pltpu
from jax.sharding import PartitionSpec as P

NW = 7
LOCAL = 5
MESH = pl.DeviceIdType.MESH
F32 = jnp.float32
BF16 = jnp.bfloat16


def remote(src, dst, send_sem, recv_sem, device):
    return pltpu.make_async_remote_copy(
        src_ref=src,
        dst_ref=dst,
        send_sem=send_sem,
        recv_sem=recv_sem,
        device_id=device,
        device_id_type=MESH,
    )


class Phases:
    def __init__(self):
        self.open = None

    def __call__(self, name):
        if self.open is not None:
            self.open.__exit__(None, None, None)
        self.open = jax.named_scope(name) if name else None
        if self.open is not None:
            self.open.__enter__()


def contract(a, b, da, db):
    return lax.dot_general(a, b, (((da,), (db,)), ((), ())), preferred_element_type=F32)


def softmax_terms(score, pos, count, scale, weight):
    logit = jnp.where(count > 0.0, score * scale, -jnp.inf)
    pos_logit = pos * scale
    highest = jnp.maximum(jnp.max(logit, axis=1, keepdims=True), pos_logit)
    neg_exp = count * jnp.exp(logit - highest)
    pos_exp = jnp.exp(pos_logit - highest)
    denominator = jnp.sum(neg_exp, axis=1, keepdims=True) + pos_exp
    row_weight = weight * scale
    return neg_exp * (row_weight / denominator), row_weight * (pos_exp / denominator - 1.0)


def kernel(
    scale_hbm, loss_hbm, short_hbm, send_hbm, q_hbm, d_hbm, head_hbm,
    qg_ref, dg_ref, hg_ref,
    scale_ref, loss_ref, short_ref, send_ref, rows, head, rows_t, rt_buf, grads_0, grads_1,
    out_buf, fetched, back_buf, returned,
    score_buf, part_q, got_q, part_d, got_d,
    full_0, full_1, part_0, part_1, got_0, got_1,
    load_sem, ag_s, ag_r, fe_s, fe_r, sc_s, sc_r, rt_s, rt_r, ba_s, ba_r,
    gr_s, gr_r, pq_s, pq_r, pd_s, pd_r, hg_s, hg_r, word,
):
    n_dp, n_mp, ql, cols = 32, 4, 64, 640
    group = 8
    slots = 128
    block = 4
    hrows = 80
    cuts = (0, 384, cols)
    grads, full_h, part_h, got_h = (
        (grads_0, grads_1), (full_0, full_1), (part_0, part_1), (got_0, got_1)
    )
    me = lax.axis_index("dp")
    my = lax.axis_index("mp")
    x = me // group
    g = me % group
    z = g // 2
    feature_total = n_mp * cols
    bounds = [0] + [feature_total // 2 ** (NW - 1 - w) for w in range(NW)]

    def row_block(m):
        return pl.ds(pl.multiple_of(m * cols, cols), cols)

    phase = Phases()
    phase("loads")
    load_q = pltpu.make_async_copy(q_hbm, rows.at[my, pl.ds(0, ql)], load_sem.at[0])
    load_d = pltpu.make_async_copy(d_hbm, rows.at[my, pl.ds(ql, ql)], load_sem.at[1])
    load_short = pltpu.make_async_copy(short_hbm, short_ref, load_sem.at[6])
    load_send = pltpu.make_async_copy(send_hbm, send_ref, load_sem.at[7])
    load_loss = pltpu.make_async_copy(loss_hbm, loss_ref, load_sem.at[8])
    load_scale = pltpu.make_async_copy(scale_hbm, scale_ref, load_sem.at[9])
    load_d.start()
    load_q.start()
    load_short.start()
    load_send.start()
    load_loss.start()
    load_scale.start()
    order = (0, 1, 3, 2)
    load_h = []
    for k in order:
        src = (my + n_mp - k) % n_mp
        copy = pltpu.make_async_copy(
            head_hbm.at[row_block(src)], head.at[row_block(src)], load_sem.at[2 + k]
        )
        copy.start()
        load_h.append(copy)

    phase("greet")
    right, left = (my + 1) % n_mp, (my + n_mp - 1) % n_mp
    far = (my + 2) % n_mp
    core = me % 2
    partner = me + 1 - 2 * core
    x_near = ((me + group) % n_dp, (me + n_dp - group) % n_dp)
    z_near = (x * group + (g + 2) % group, x * group + (g + 6) % group)
    barrier = pltpu.get_barrier_semaphore()
    near = [(me, right), (me, left), (me, far), (partner, my)]
    near += [(peer, my) for peer in x_near + z_near]
    for device in near:
        pl.semaphore_signal(barrier, inc=1, device_id=device, device_id_type=MESH)

    def await_sent(ref, sem):
        remote(ref, ref, sem, sem, (me, my)).wait_send()

    def await_got(ref, sem):
        remote(ref, ref, sem, sem, (me, my)).wait_recv()

    steps = [(i, j, k) for i in (2, 1, 3, 0) for j in (2, 1, 3, 0) for k in (0, 1)]
    steps.sort(key=lambda d: -(min(d[0], 4 - d[0]) + min(d[1], 4 - d[1])))
    others = [
        ((x + i) % 4 * group + (z + j) % 4 * 2 + (core if k == 0 else 1 - core))
        for i, j, k in steps
        if (i, j, k) != (0, 0, 0)
    ]

    def tell(step, peers):
        for peer in peers:
            pl.semaphore_signal(
                word.at[step], inc=1, device_id=(peer, my), device_id_type=MESH
            )

    def hear(step, count):
        pl.semaphore_wait(word.at[step], count)

    load_d.wait()
    pl.semaphore_wait(barrier, len(near))

    half, quarter = ql // 2, ql // 4

    def row_copy(part, slot, src):
        first, count, peer = (
            (0, half, far),
            (0, ql, right),
            (half, quarter, left),
            (half + quarter, quarter, left),
            (0, half, left),
            (half, quarter, left),
            (half + quarter, quarter, left),
        )[slot]
        at = pl.ds((1 - part) * ql + first, count)
        slot = part * 7 + slot
        return remote(
            rows.at[src, at], rows.at[src, at], ag_s, ag_r.at[slot], (me, peer)
        )

    def rows_start(part):
        for slot in (0, 2, 1, 3, 4):
            row_copy(part, slot, my).start()

    def rows_relay(part):
        for slot in (2, 3):
            row_copy(part, slot, right).wait_recv()
            row_copy(part, slot + 3, right).start()

    def rows_right(part):
        row_copy(part, 4, right).wait_recv()
        return product_of(part, right)

    def rows_left(part):
        row_copy(part, 1, left).wait_recv()
        return product_of(part, left)

    def rows_far(part):
        for slot in (0, 5, 6):
            row_copy(part, slot, far).wait_recv()
        return product_of(part, far)

    def product_of(part, src):
        at = (1 - part) * ql
        return jnp.dot(
            rows[src, at : at + ql, :], head[row_block(src), :], preferred_element_type=F32
        )

    home = (1, 0)
    chips = (z, x)
    spots = (x, z)

    def gatherer(axis, pos):
        return x * group + pos * 2 + home[0] if axis == 0 else pos * group + z * 2 + home[1]

    def reducer(axis, pos, c):
        return pos * group + z * 2 + c if axis == 0 else x * group + pos * 2 + c

    def items(axis):
        return chips[axis] * 2 + core

    def turned(axis, pos):
        return rows_t.at[:, pos] if axis == 0 else rows_t.at[pos]

    def turn_rows():
        for m in range(n_mp):
            rows_t[m] = rows[m].T.reshape(n_mp, 2, hrows, slots)

    def turn_start(axes):
        for axis in axes:
            at = pl.ds(pl.multiple_of(items(axis) * slots, slots), slots)
            for k in (2, 1, 3):
                pos = (chips[axis] + k) % n_mp
                remote(
                    turned(axis, pos), rt_buf.at[:, :, :, at], rt_s, rt_r,
                    (gatherer(axis, pos), my),
                ).start()

            @pl.when(core == home[axis])
            def _():
                rt_buf[:, :, :, at] = turned(axis, chips[axis])[...]

            @pl.when(core != home[axis])
            def _():
                remote(
                    turned(axis, chips[axis]), rt_buf.at[:, :, :, at], rt_s, rt_r, (partner, my)
                ).start()

    rt_others = rt_buf.at[:, :, :, pl.ds(0, (group - 1) * slots)]

    phase("rows_d")
    rows_start(0)
    tell(0, x_near)
    load_h[0].wait()
    acc = product_of(0, my)
    load_send.wait()
    pick = jnp.where(
        lax.broadcasted_iota(jnp.int32, (ql, slots), 0) == send_ref[...], 1.0, 0.0
    ).astype(BF16)

    for copy in load_h[1:]:
        copy.wait()
    hear(0, 2)
    tell(1, z_near)
    phase("relay_d")
    rows_relay(0)
    load_q.wait()
    rows_start(1)
    hear(1, 2)
    tell(2, z_near)
    phase("right_d")
    acc = acc + rows_right(0)
    hear(2, 2)
    tell(3, (partner,))
    phase("left_d")
    acc = acc + rows_left(0)
    phase("far_d")
    acc = acc + rows_far(0)
    hear(3, 1)
    phase("pick")
    dp = acc.astype(BF16)

    picked = contract(pick, dp, 0, 0).astype(BF16)
    out_buf[...] = picked.reshape(n_dp, block, cols)

    phase("fetch")
    for peer in others:
        remote(out_buf.at[peer], fetched.at[me], fe_s, fe_r, (peer, my)).start()
    fetched[me] = out_buf[me]

    phase("relay_q")
    rows_relay(1)
    phase("count")
    load_loss.wait()
    load_scale.wait()
    weight = loss_ref[...].T
    load_short.wait()
    short = short_ref[...]
    lane = lax.broadcasted_iota(jnp.int32, (ql, slots), 1)

    count = jnp.zeros((ql, slots), F32)
    for k in range(slots):
        count = count + jnp.where((short if k == 0 else pltpu.roll(short, k, 1)) == lane, 1.0, 0.0)
    phase("rows_q")
    acc = product_of(1, my) + rows_right(1) + rows_left(1) + rows_far(1)
    qp = acc.astype(BF16)

    phase("turn0")
    turn_rows()
    turn_start((0,))
    phase("mask")
    col = lax.broadcasted_iota(jnp.int32, (1, cols), 1)
    seg_col = [
        jnp.where((col >= bounds[s]) & (col < bounds[s + 1]), 1.0, 0.0) for s in range(LOCAL)
    ]
    q_seg = jnp.concatenate([qp * m.astype(BF16) for m in seg_col], axis=0)
    product = qp.astype(F32) * dp.astype(F32)
    pos_prefix = [
        jnp.sum(
            product * jnp.where(col < bounds[s + 1], 1.0, 0.0), axis=1, keepdims=True
        )
        for s in range(LOCAL)
    ]

    phase("fetch_wait")
    await_got(fetched.at[pl.ds(0, n_dp - 1)], fe_r)
    phase("turn")
    turn_start((1,))
    phase("score")
    docs = fetched[...].reshape(slots, cols)
    pieces = contract(q_seg, docs, 1, 1)
    scores = []
    for s in range(LOCAL):
        piece = pieces[s * ql : (s + 1) * ql]
        scores.append(piece if s == 0 else scores[-1] + piece)

    diag = lax.broadcasted_iota(jnp.int32, (ql, slots), 0) == lane
    pos_row = jnp.sum(
        jnp.where(diag, jnp.broadcast_to(pos_prefix[-1], (ql, slots)), 0.0), axis=0, keepdims=True
    )
    score_buf[my, 0:ql, :] = scores[-1]
    score_buf[my, ql : ql + 8, :] = jnp.broadcast_to(pos_row, (8, slots))
    for peer in (far, right, left):
        remote(score_buf.at[my], score_buf.at[my], sc_s, sc_r, (me, peer)).start()

    phase("narrow")
    def width(w, score, pos):
        scale = scale_ref[w] * (1.0 / math.sqrt(bounds[w + 1]))
        return softmax_terms(score, pos, count, scale, weight[:, w : w + 1])

    narrow = [width(w, scores[w], pos_prefix[w]) for w in range(LOCAL)]
    doc_seg = [docs * m.astype(BF16) for m in seg_col]
    wide_at = 256
    docs_low = jnp.concatenate([m[:, :wide_at] for m in doc_seg[:4]], axis=0)
    docs_high = jnp.concatenate([m[:, wide_at:] for m in doc_seg[3:]], axis=0)

    phase("score_wait")
    await_got(score_buf.at[pl.ds(0, n_mp - 1)], sc_r)
    phase("wide")
    parts = [score_buf[m, 0:ql, :] for m in range(n_mp)]
    pos_parts = [
        jnp.sum(
            jnp.where(diag, jnp.concatenate([score_buf[m, ql : ql + 8, :]] * 8, axis=0), 0.0),
            axis=1,
            keepdims=True,
        )
        for m in range(n_mp)
    ]
    score5, pos5 = parts[0] + parts[1], pos_parts[0] + pos_parts[1]
    neg5, posg5 = width(5, score5, pos5)
    neg6, posg6 = width(6, score5 + (parts[2] + parts[3]), pos5 + (pos_parts[2] + pos_parts[3]))
    run_neg = neg6 + jnp.where(my <= 1, neg5, 0.0)
    run_pos = posg6 + jnp.where(my <= 1, posg5, 0.0)
    coeff = [None] * LOCAL
    pos_cols = jnp.zeros((ql, cols), F32)
    for s in reversed(range(LOCAL)):
        run_neg = run_neg + jnp.where(my == 0, narrow[s][0], 0.0)
        run_pos = run_pos + jnp.where(my == 0, narrow[s][1], 0.0)
        coeff[s] = run_neg.astype(BF16)
        pos_cols = pos_cols + run_pos * seg_col[s]

    phase("by_slot")
    by_slot = jnp.concatenate(
        [
            contract(jnp.concatenate(coeff[:4], axis=0), q_seg[: 4 * ql, :wide_at], 0, 0),
            contract(jnp.concatenate(coeff[3:], axis=0), q_seg[3 * ql :, wide_at:], 0, 0),
        ],
        axis=1,
    ).astype(BF16)
    back_buf[...] = by_slot.reshape(n_dp, block, cols)

    for peer in others:
        remote(back_buf.at[peer], returned.at[me], ba_s, ba_r, (peer, my)).start()
    returned[me] = back_buf[me]

    phase("grad_q")
    query_back = jnp.concatenate(
        [
            jnp.dot(jnp.concatenate(coeff[:4], axis=1), docs_low, preferred_element_type=F32),
            jnp.dot(jnp.concatenate(coeff[3:], axis=1), docs_high, preferred_element_type=F32),
        ],
        axis=1,
    )
    grad_q = (query_back + pos_cols * dp.astype(F32)).astype(BF16)

    def spread(part, grad):
        for axis in range(2):
            at = pl.ds(pl.multiple_of(items(axis) * slots + part * ql, ql), ql)
            grads[axis][at, :] = grad[:, cuts[axis] : cuts[axis + 1]]
        for k in (2, 1, 3, 0):
            for axis in range(2):
                at = pl.ds(pl.multiple_of(items(axis) * slots + part * ql, ql), ql)
                ref = grads[axis].at[at]
                if k:
                    device = gatherer(axis, (chips[axis] + k) % n_mp)
                    remote(ref, ref, gr_s.at[axis], gr_r.at[k], (device, my)).start()
                else:

                    @pl.when(core != home[axis])
                    def _():
                        remote(ref, ref, gr_s.at[axis], gr_r.at[0], (partner, my)).start()

    def share(grad, part, got, send_sem, recv_sem):
        for k in (2, 1, 3):
            peer = (my + k) % n_mp
            part[k] = contract(grad, head[row_block(peer), :], 1, 1).astype(BF16)
            remote(part.at[k], got.at[k], send_sem, recv_sem, (me, peer)).start()
        return contract(grad, head[row_block(my), :], 1, 1)

    def gather_parts(own, got):
        for k in (1, 3, 2):
            own = own + got[k].astype(F32)
        return own

    phase("share_q")
    own_q = share(grad_q, part_q, got_q, pq_s, pq_r)

    phase("spread_q")
    spread(0, grad_q)
    phase("back_wait")
    await_got(returned.at[pl.ds(0, n_dp - 1)], ba_r)
    phase("grad_d")
    doc_back = jnp.dot(pick, returned[...].reshape(slots, cols), preferred_element_type=F32)
    grad_d = (pos_cols * qp.astype(F32) + doc_back).astype(BF16)
    spread(1, grad_d)
    phase("share_d")
    own_d = share(grad_d, part_d, got_d, pd_s, pd_r)
    phase("rt_wait")
    await_got(rt_others, rt_r)
    phase(None)

    def head_part(axis):
        def arrived(k):
            await_got(grads[axis].at[pl.ds(0, (4 if k else 2) * ql)], gr_r.at[k])
            pos = (chips[axis] + n_mp - k) % n_mp
            at = pl.ds(pl.multiple_of(pos * 2 * slots, 2 * slots), 2 * slots)
            return jnp.dot(
                rt_buf[:, :, :, at].reshape(8 * hrows, 2 * slots), grads[axis][at, :],
                preferred_element_type=F32,
            )

        total = None
        for k in (0, 1, 3, 2):
            with jax.named_scope("chip_h"):
                term = arrived(k)
                total = term if total is None else total + term
        with jax.named_scope("head"):
            full_h[axis][...] = total.reshape(8, hrows, -1)
            part_h[axis][...] = full_h[axis][...].astype(BF16)
            for k in (2, 1, 3):
                pos = (spots[axis] + k) % n_mp
                for c in range(2):
                    remote(
                        part_h[axis].at[pos * 2 + c], got_h[axis].at[k],
                        hg_s.at[axis], hg_r.at[axis], (reducer(axis, pos, c), my),
                    ).start()
            remote(
                part_h[axis].at[spots[axis] * 2 + 1 - home[axis]], got_h[axis].at[0],
                hg_s.at[axis], hg_r.at[axis], (partner, my),
            ).start()

    for axis in range(2):
        pl.when(core == home[axis])(functools.partial(head_part, axis))
    phase("query_out")
    await_got(got_q.at[pl.ds(1, n_mp - 1)], pq_r)
    qg_ref[...] = gather_parts(own_q, got_q).astype(BF16)

    phase("doc_out")
    await_got(got_d.at[pl.ds(1, n_mp - 1)], pd_r)
    dg_ref[...] = gather_parts(own_d, got_d).astype(BF16)
    phase("head_out")
    for axis in range(2):
        columns = slice(cuts[axis], cuts[axis + 1])

        @pl.when(core == home[axis])
        def _():
            await_got(got_h[axis].at[pl.ds(1, n_mp - 1)], hg_r.at[axis])
            mine = full_h[axis][spots[axis] * 2 + home[axis]]
            hg_ref[:, columns] = gather_parts(mine, got_h[axis])

        @pl.when(core != home[axis])
        def _():
            await_got(got_h[axis], hg_r.at[axis])
            hg_ref[:, columns] = gather_parts(got_h[axis][0].astype(F32), got_h[axis])

    phase("drain")
    await_sent(rows.at[pl.ds(0, 3)], ag_s)
    await_sent(out_buf.at[pl.ds(0, n_dp - 1)], fe_s)
    await_sent(rt_others, rt_s)
    await_sent(score_buf.at[pl.ds(0, n_mp - 1)], sc_s)
    await_sent(back_buf.at[pl.ds(0, n_dp - 1)], ba_s)
    for axis in range(2):

        @pl.when(core == home[axis])
        def _():
            await_sent(grads[axis].at[pl.ds(0, 6 * ql)], gr_s.at[axis])
            await_sent(part_h[axis].at[pl.ds(0, 7)], hg_s.at[axis])

        @pl.when(core != home[axis])
        def _():
            await_sent(grads[axis].at[pl.ds(0, 8 * ql)], gr_s.at[axis])

    await_sent(part_q.at[pl.ds(1, n_mp - 1)], pq_s)
    await_sent(part_d.at[pl.ds(1, n_mp - 1)], pd_s)
    phase(None)


def hand_out(a, b, c, out_a, out_b, out_c, sem):
    copies = [
        pltpu.make_async_copy(src, dst, sem.at[i])
        for i, (src, dst) in enumerate(((c, out_c), (a, out_a), (b, out_b)))
    ]
    for copy in copies:
        copy.start()
    for copy in copies:
        copy.wait()


def on_device(query_rows, doc_rows, head, logit_scale, loss_grad, shortlist, send_rows):
    ql, cols = query_rows.shape
    dma = pltpu.SemaphoreType.DMA
    one = dma(())
    hbm = pl.BlockSpec(memory_space=pltpu.HBM)
    vmem = pl.BlockSpec(memory_space=pltpu.VMEM)
    operands = (logit_scale, loss_grad.T, shortlist, send_rows, query_rows, doc_rows, head)
    shapes = (
        jax.ShapeDtypeStruct((ql, cols), BF16),
        jax.ShapeDtypeStruct((ql, cols), BF16),
        jax.ShapeDtypeStruct((80, cols), F32),
    )
    results = pl.pallas_call(
        kernel,
        out_shape=shapes,
        in_specs=[hbm] * 7,
        out_specs=(vmem, vmem, vmem),
        scratch_shapes=[
            pltpu.SMEM((NW,), F32),
            pltpu.VMEM((NW, ql), F32),
            pltpu.VMEM((ql, 128), jnp.int32),
            pltpu.VMEM((1, 128), jnp.int32),
            pltpu.VMEM((4, 2 * ql, cols), BF16),
            pltpu.VMEM((4 * cols, cols), BF16),
            pltpu.VMEM((4, 4, 2, 80, 128), BF16),
            pltpu.VMEM((4, 2, 80, 1024), BF16),
            pltpu.VMEM((1024, 384), BF16),
            pltpu.VMEM((1024, 256), BF16),
            pltpu.VMEM((32, 4, cols), BF16),
            pltpu.VMEM((32, 4, cols), BF16),
            pltpu.VMEM((32, 4, cols), BF16),
            pltpu.VMEM((32, 4, cols), BF16),
            pltpu.VMEM((4, ql + 8, 128), F32),
            pltpu.VMEM((4, ql, cols), BF16),
            pltpu.VMEM((4, ql, cols), BF16),
            pltpu.VMEM((4, ql, cols), BF16),
            pltpu.VMEM((4, ql, cols), BF16),
            pltpu.VMEM((8, 80, 384), F32),
            pltpu.VMEM((8, 80, 256), F32),
            pltpu.VMEM((8, 80, 384), BF16),
            pltpu.VMEM((8, 80, 256), BF16),
            pltpu.VMEM((4, 80, 384), BF16),
            pltpu.VMEM((4, 80, 256), BF16),
            dma((10,)), one, dma((14,)), one, one, one, one, one, one, one, one,
            dma((2,)), dma((4,)), one, one, one, one, dma((2,)), dma((2,)),
            pltpu.SemaphoreType.REGULAR((4,)),
        ],
        compiler_params=pltpu.CompilerParams(
            collective_id=0, has_side_effects=True, vmem_limit_bytes=48 * 1024 * 1024
        ),
    )(*[pltpu.with_memory_space_constraint(a, pltpu.HBM) for a in operands])
    anywhere = pl.BlockSpec(memory_space=pl.ANY)
    return pl.pallas_call(
        hand_out,
        out_shape=shapes,
        in_specs=[anywhere] * 3,
        out_specs=(anywhere,) * 3,
        scratch_shapes=[dma((3,))],
        compiler_params=pltpu.CompilerParams(vmem_limit_bytes=1024 * 1024),
    )(*results)


def solution(mesh):
    placed = (
        P("dp", "mp"),
        P("dp", "mp"),
        P(None, "mp"),
        P(),
        P("dp", None),
        P("dp", None),
        P("dp", None),
    )
    return jax.shard_map(
        on_device,
        mesh=mesh,
        in_specs=placed,
        out_specs=(P("dp", "mp"), P("dp", "mp"), P("dp", "mp")),
        check_vma=False,
    )
```

```python
import functools
import math

import jax
import jax.numpy as jnp
from jax import lax
from jax.experimental import pallas as pl
from jax.experimental.pallas import tpu as pltpu
from jax.sharding import PartitionSpec as P

NW = 7
LOCAL = 5
MESH = pl.DeviceIdType.MESH
F32 = jnp.float32
BF16 = jnp.bfloat16


def remote(src, dst, send_sem, recv_sem, device):
    return pltpu.make_async_remote_copy(
        src_ref=src,
        dst_ref=dst,
        send_sem=send_sem,
        recv_sem=recv_sem,
        device_id=device,
        device_id_type=MESH,
    )


class Phases:
    def __init__(self):
        self.open = None

    def __call__(self, name):
        if self.open is not None:
            self.open.__exit__(None, None, None)
        self.open = jax.named_scope(name) if name else None
        if self.open is not None:
            self.open.__enter__()


def contract(a, b, da, db):
    return lax.dot_general(a, b, (((da,), (db,)), ((), ())), preferred_element_type=F32)


def softmax_terms(score, pos, count, scale, weight):
    logit = jnp.where(count > 0.0, score * scale, -jnp.inf)
    pos_logit = pos * scale
    highest = jnp.maximum(jnp.max(logit, axis=1, keepdims=True), pos_logit)
    neg_exp = count * jnp.exp(logit - highest)
    pos_exp = jnp.exp(pos_logit - highest)
    denominator = jnp.sum(neg_exp, axis=1, keepdims=True) + pos_exp
    row_weight = weight * scale
    return neg_exp * (row_weight / denominator), row_weight * (pos_exp / denominator - 1.0)


def kernel(
    scale_hbm, loss_hbm, short_hbm, send_hbm, q_hbm, d_hbm, head_hbm,
    qg_ref, dg_ref, hg_ref,
    scale_ref, loss_ref, short_ref, send_ref, rows, head, rows_t, rt_buf, grads_0, grads_1,
    out_buf, fetched, back_buf, returned,
    score_buf, part_q, got_q, part_d, got_d,
    full_0, full_1, part_0, part_1, got_0, got_1,
    load_sem, ag_s, ag_r, fe_s, fe_r, sc_s, sc_r, rt_s, rt_r, ba_s, ba_r,
    gr_s, gr_r, pq_s, pq_r, pd_s, pd_r, hg_s, hg_r, word,
):
    n_dp, n_mp, ql, cols = 32, 4, 64, 640
    group = 8
    slots = 128
    block = 4
    hrows = 80
    cuts = (0, 384, cols)
    grads, full_h, part_h, got_h = (
        (grads_0, grads_1), (full_0, full_1), (part_0, part_1), (got_0, got_1)
    )
    me = lax.axis_index("dp")
    my = lax.axis_index("mp")
    x = me // group
    g = me % group
    z = g // 2
    feature_total = n_mp * cols
    bounds = [0] + [feature_total // 2 ** (NW - 1 - w) for w in range(NW)]

    def row_block(m):
        return pl.ds(pl.multiple_of(m * cols, cols), cols)

    phase = Phases()
    phase("loads")
    load_q = pltpu.make_async_copy(q_hbm, rows.at[my, pl.ds(0, ql)], load_sem.at[0])
    load_d = pltpu.make_async_copy(d_hbm, rows.at[my, pl.ds(ql, ql)], load_sem.at[1])
    load_short = pltpu.make_async_copy(short_hbm, short_ref, load_sem.at[6])
    load_send = pltpu.make_async_copy(send_hbm, send_ref, load_sem.at[7])
    load_loss = pltpu.make_async_copy(loss_hbm, loss_ref, load_sem.at[8])
    load_scale = pltpu.make_async_copy(scale_hbm, scale_ref, load_sem.at[9])
    load_d.start()
    load_q.start()
    load_short.start()
    load_send.start()
    load_loss.start()
    load_scale.start()
    order = (0, 1, 3, 2)
    load_h = []
    for k in order:
        src = (my + n_mp - k) % n_mp
        copy = pltpu.make_async_copy(
            head_hbm.at[row_block(src)], head.at[row_block(src)], load_sem.at[2 + k]
        )
        copy.start()
        load_h.append(copy)

    phase("greet")
    right, left = (my + 1) % n_mp, (my + n_mp - 1) % n_mp
    far = (my + 2) % n_mp
    core = me % 2
    partner = me + 1 - 2 * core
    x_near = ((me + group) % n_dp, (me + n_dp - group) % n_dp)
    z_near = (x * group + (g + 2) % group, x * group + (g + 6) % group)
    barrier = pltpu.get_barrier_semaphore()
    near = [(me, right), (me, left), (me, far), (partner, my)]
    near += [(peer, my) for peer in x_near + z_near]
    for device in near:
        pl.semaphore_signal(barrier, inc=1, device_id=device, device_id_type=MESH)

    def await_sent(ref, sem):
        remote(ref, ref, sem, sem, (me, my)).wait_send()

    def await_got(ref, sem):
        remote(ref, ref, sem, sem, (me, my)).wait_recv()

    steps = [(i, j, k) for i in (2, 1, 3, 0) for j in (2, 1, 3, 0) for k in (0, 1)]
    steps.sort(key=lambda d: -(min(d[0], 4 - d[0]) + min(d[1], 4 - d[1])))
    others = [
        ((x + i) % 4 * group + (z + j) % 4 * 2 + (core if k == 0 else 1 - core))
        for i, j, k in steps
        if (i, j, k) != (0, 0, 0)
    ]

    def tell(step, peers):
        for peer in peers:
            pl.semaphore_signal(
                word.at[step], inc=1, device_id=(peer, my), device_id_type=MESH
            )

    def hear(step, count):
        pl.semaphore_wait(word.at[step], count)

    load_d.wait()
    pl.semaphore_wait(barrier, len(near))

    half, quarter = ql // 2, ql // 4
    row_pieces = (
        (0, half, far),
        (half, quarter, right),
        (half + quarter, quarter, right),
        (0, half, right),
        (half + quarter, quarter, left),
        (0, half + quarter, left),
        (half, quarter, right),
        (half + quarter, quarter, left),
    )

    def row_copy(part, slot, src):
        first, count, peer = row_pieces[slot]
        at = pl.ds((1 - part) * ql + first, count)
        slot = part * 8 + slot
        return remote(
            rows.at[src, at], rows.at[src, at], ag_s, ag_r.at[slot], (me, peer)
        )

    def rows_start(part):
        for slot in (1, 4, 0, 2, 3, 5):
            row_copy(part, slot, my).start()

    def rows_relay(part):
        for slot, src in ((1, left), (4, right)):
            row_copy(part, slot, src).wait_recv()
            row_copy(part, 6 if slot == 1 else 7, src).start()

    def rows_right(part):
        row_copy(part, 5, right).wait_recv()
        return product_of(part, right)

    def rows_left(part):
        for slot in (2, 3):
            row_copy(part, slot, left).wait_recv()
        return product_of(part, left)

    def rows_far(part):
        for slot in (0, 6, 7):
            row_copy(part, slot, far).wait_recv()
        return product_of(part, far)

    def product_of(part, src):
        at = (1 - part) * ql
        return jnp.dot(
            rows[src, at : at + ql, :], head[row_block(src), :], preferred_element_type=F32
        )

    home = (1, 0)
    chips = (z, x)
    spots = (x, z)

    bands = (((0, 384),), ((0, 256),))

    def gatherer(axis, pos):
        return x * group + pos * 2 + home[0] if axis == 0 else pos * group + z * 2 + home[1]

    def reducer(axis, pos, c):
        return pos * group + z * 2 + c if axis == 0 else x * group + pos * 2 + c

    def place(k):
        return pl.multiple_of(k * 2 * slots + core * slots, slots)

    def turned(axis, pos):
        return rows_t.at[:, pos] if axis == 0 else rows_t.at[pos]

    def turn_rows():
        for m in range(n_mp):
            rows_t[m] = rows[m].T.reshape(n_mp, 2, hrows, slots)

    def turn_start(axes):
        for axis in axes:
            own = pl.ds(place(0), slots)
            for k in (2, 1, 3):
                pos = (chips[axis] + k) % n_mp
                remote(
                    turned(axis, pos), rt_buf.at[:, :, :, pl.ds(place(k), slots)], rt_s, rt_r,
                    (gatherer(axis, pos), my),
                ).start()

            @pl.when(core == home[axis])
            def _():
                rt_buf[:, :, :, own] = turned(axis, chips[axis])[...]

            @pl.when(core != home[axis])
            def _():
                remote(
                    turned(axis, chips[axis]), rt_buf.at[:, :, :, own], rt_s, rt_r, (partner, my)
                ).start()

    rt_others = rt_buf.at[:, :, :, pl.ds(0, (group - 1) * slots)]

    phase("rows_d")
    rows_start(0)
    tell(0, x_near)
    load_h[0].wait()
    acc = product_of(0, my)
    load_send.wait()
    pick = jnp.where(
        lax.broadcasted_iota(jnp.int32, (ql, slots), 0) == send_ref[...], 1.0, 0.0
    ).astype(BF16)

    for copy in load_h[1:]:
        copy.wait()
    hear(0, 2)
    tell(1, z_near)
    phase("relay_d")
    rows_relay(0)
    load_q.wait()
    rows_start(1)
    hear(1, 2)
    tell(2, z_near)
    phase("right_d")
    acc = acc + rows_right(0)
    hear(2, 2)
    tell(3, (partner,))
    phase("left_d")
    acc = acc + rows_left(0)
    phase("far_d")
    acc = acc + rows_far(0)
    hear(3, 1)
    phase("pick")
    dp = acc.astype(BF16)

    picked = contract(pick, dp, 0, 0).astype(BF16)
    out_buf[...] = picked.reshape(n_dp, block, cols)

    phase("fetch")
    for peer in others:
        remote(out_buf.at[peer], fetched.at[me], fe_s, fe_r, (peer, my)).start()
    fetched[me] = out_buf[me]

    phase("relay_q")
    rows_relay(1)
    phase("count")
    load_loss.wait()
    load_scale.wait()
    weight = loss_ref[...].T
    load_short.wait()
    short = short_ref[...]
    lane = lax.broadcasted_iota(jnp.int32, (ql, slots), 1)

    count = jnp.zeros((ql, slots), F32)
    for k in range(slots):
        count = count + jnp.where((short if k == 0 else pltpu.roll(short, k, 1)) == lane, 1.0, 0.0)
    phase("rows_q")
    acc = product_of(1, my) + rows_right(1) + rows_left(1) + rows_far(1)
    qp = acc.astype(BF16)

    phase("turn0")
    turn_rows()
    turn_start((1, 0))
    phase("mask")
    col = lax.broadcasted_iota(jnp.int32, (1, cols), 1)
    seg_col = [
        jnp.where((col >= bounds[s]) & (col < bounds[s + 1]), 1.0, 0.0) for s in range(LOCAL)
    ]
    q_seg = jnp.concatenate([qp * m.astype(BF16) for m in seg_col], axis=0)
    product = qp.astype(F32) * dp.astype(F32)
    pos_prefix = [
        jnp.sum(
            product * jnp.where(col < bounds[s + 1], 1.0, 0.0), axis=1, keepdims=True
        )
        for s in range(LOCAL)
    ]

    diag = lax.broadcasted_iota(jnp.int32, (ql, slots), 0) == lane
    pos_row = jnp.sum(
        jnp.where(diag, jnp.broadcast_to(pos_prefix[-1], (ql, slots)), 0.0), axis=0, keepdims=True
    )
    score_buf[my, ql : ql + 8, :] = jnp.broadcast_to(pos_row, (8, slots))

    phase("fetch_wait")
    await_got(fetched.at[pl.ds(0, n_dp - 1)], fe_r)
    phase("score")
    docs = fetched[...].reshape(slots, cols)
    whole = contract(qp, docs, 1, 1)
    score_buf[my, 0:ql, :] = whole
    for peer in (far, right, left):
        remote(score_buf.at[my], score_buf.at[my], sc_s, sc_r, (me, peer)).start()

    phase("narrow")
    def width(w, score, pos):
        scale = scale_ref[w] * (1.0 / math.sqrt(bounds[w + 1]))
        return softmax_terms(score, pos, count, scale, weight[:, w : w + 1])

    pieces = contract(q_seg[: 4 * ql], docs, 1, 1)
    scores = []
    for s in range(LOCAL - 1):
        piece = pieces[s * ql : (s + 1) * ql]
        scores.append(piece if s == 0 else scores[-1] + piece)
    scores.append(whole)
    narrow = [width(w, scores[w], pos_prefix[w]) for w in range(LOCAL)]
    for s in reversed(range(LOCAL - 1)):
        narrow[s] = tuple(a + b for a, b in zip(narrow[s], narrow[s + 1]))
    narrow = [tuple(jnp.where(my == 0, a, 0.0) for a in terms) for terms in narrow]
    doc_seg = [docs * m.astype(BF16) for m in seg_col]
    wide_at = 256
    docs_low = jnp.concatenate([m[:, :wide_at] for m in doc_seg[:4]], axis=0)
    docs_high = jnp.concatenate([m[:, wide_at:] for m in doc_seg[3:]], axis=0)

    phase("score_wait")
    await_got(score_buf.at[pl.ds(0, n_mp - 1)], sc_r)
    phase("wide")
    parts = [score_buf[m, 0:ql, :] for m in range(n_mp)]
    pos_rows = [score_buf[m, ql : ql + 8, :] for m in range(n_mp)]
    pos_row5 = pos_rows[0] + pos_rows[1]
    pos5, pos6 = [
        jnp.sum(
            jnp.where(diag, jnp.concatenate([row] * 8, axis=0), 0.0), axis=1, keepdims=True
        )
        for row in (pos_row5, pos_row5 + (pos_rows[2] + pos_rows[3]))
    ]
    score5 = parts[0] + parts[1]
    neg5, posg5 = width(5, score5, pos5)
    neg6, posg6 = width(6, score5 + (parts[2] + parts[3]), pos6)
    run_neg = neg6 + jnp.where(my <= 1, neg5, 0.0)
    run_pos = posg6 + jnp.where(my <= 1, posg5, 0.0)
    coeff = [(run_neg + narrow[s][0]).astype(BF16) for s in range(LOCAL)]

    phase("by_slot")
    by_slot = jnp.concatenate(
        [
            contract(jnp.concatenate(coeff[:4], axis=0), q_seg[: 4 * ql, :wide_at], 0, 0),
            contract(jnp.concatenate(coeff[3:], axis=0), q_seg[3 * ql :, wide_at:], 0, 0),
        ],
        axis=1,
    ).astype(BF16)
    back_buf[...] = by_slot.reshape(n_dp, block, cols)

    for peer in others:
        remote(back_buf.at[peer], returned.at[me], ba_s, ba_r, (peer, my)).start()
    returned[me] = back_buf[me]

    phase("grad_q")
    pos_cols = (run_pos + narrow[0][1]) * seg_col[0]
    for s in range(1, LOCAL):
        pos_cols = pos_cols + (run_pos + narrow[s][1]) * seg_col[s]
    query_back = jnp.concatenate(
        [
            jnp.dot(jnp.concatenate(coeff[:4], axis=1), docs_low, preferred_element_type=F32),
            jnp.dot(jnp.concatenate(coeff[3:], axis=1), docs_high, preferred_element_type=F32),
        ],
        axis=1,
    )
    grad_q = (query_back + pos_cols * dp.astype(F32)).astype(BF16)

    def spread(part, grad):
        for axis in range(2):
            at = pl.ds(pl.multiple_of(place(0) + part * ql, ql), ql)
            grads[axis][at, :] = grad[:, cuts[axis] : cuts[axis + 1]]
        for band in range(len(bands[0])):
            for k in (2, 1, 3, 0):
                for axis in range(2):
                    columns = slice(*bands[axis][band])
                    own = pl.ds(pl.multiple_of(place(0) + part * ql, ql), ql)
                    there = pl.ds(pl.multiple_of(place(k) + part * ql, ql), ql)
                    src, dst = grads[axis].at[own, columns], grads[axis].at[there, columns]
                    if k:
                        device = gatherer(axis, (chips[axis] + k) % n_mp)
                        remote(src, dst, gr_s.at[axis], gr_r, (device, my)).start()
                    else:

                        @pl.when(core != home[axis])
                        def _():
                            remote(src, dst, gr_s.at[axis], gr_r, (partner, my)).start()

    def share(grad, part, got, send_sem, recv_sem):
        for k in (2, 1, 3):
            peer = (my + k) % n_mp
            part[k] = contract(grad, head[row_block(peer), :], 1, 1).astype(BF16)
            remote(part.at[k], got.at[k], send_sem, recv_sem, (me, peer)).start()
        return contract(grad, head[row_block(my), :], 1, 1)

    def gather_parts(own, got):
        for k in (1, 3, 2):
            own = own + got[k].astype(F32)
        return own

    phase("share_q")
    own_q = share(grad_q, part_q, got_q, pq_s, pq_r)

    phase("spread_q")
    spread(0, grad_q)
    phase("back_wait")
    await_got(returned.at[pl.ds(0, n_dp - 1)], ba_r)
    phase("grad_d")
    doc_back = jnp.dot(pick, returned[...].reshape(slots, cols), preferred_element_type=F32)
    grad_d = (pos_cols * qp.astype(F32) + doc_back).astype(BF16)
    spread(1, grad_d)
    phase("share_d")
    own_d = share(grad_d, part_d, got_d, pd_s, pd_r)
    phase("rt_wait")
    await_got(rt_others, rt_r)
    phase(None)

    def head_part(axis):
        with jax.named_scope("gather_h"):
            await_got(grads[axis].at[pl.ds(0, 7 * slots)], gr_r)
        for n in (2, 1, 3, 0):
            pos = (spots[axis] + n) % n_mp
            with jax.named_scope("head%d" % n):
                block = jnp.dot(
                    rt_buf[pos].reshape(2 * hrows, n_mp * 2 * slots), grads[axis][...],
                    preferred_element_type=F32,
                )
                part_h[axis][pl.ds(pos * 2, 2)] = block.astype(BF16).reshape(2, hrows, -1)
                if n == 0:
                    full_h[axis][...] = block[home[axis] * hrows : (home[axis] + 1) * hrows]
                    remote(
                        part_h[axis].at[pos * 2 + 1 - home[axis]], got_h[axis].at[0],
                        hg_s.at[axis], hg_r.at[axis], (partner, my),
                    ).start()
                for i in range(2 if n else 0):
                    remote(
                        part_h[axis].at[pos * 2 + i], got_h[axis].at[n],
                        hg_s.at[axis], hg_r.at[axis], (reducer(axis, pos, i), my),
                    ).start()

    for axis in range(2):
        pl.when(core == home[axis])(functools.partial(head_part, axis))
    phase("query_out")
    await_got(got_q.at[pl.ds(1, n_mp - 1)], pq_r)
    qg_ref[...] = gather_parts(own_q, got_q).astype(BF16)

    phase("doc_out")
    await_got(got_d.at[pl.ds(1, n_mp - 1)], pd_r)
    dg_ref[...] = gather_parts(own_d, got_d).astype(BF16)
    phase("head_out")
    for axis in range(2):
        columns = slice(cuts[axis], cuts[axis + 1])

        @pl.when(core == home[axis])
        def _():
            await_got(got_h[axis].at[pl.ds(1, n_mp - 1)], hg_r.at[axis])
            hg_ref[:, columns] = gather_parts(full_h[axis][...], got_h[axis])

        @pl.when(core != home[axis])
        def _():
            await_got(got_h[axis], hg_r.at[axis])
            hg_ref[:, columns] = gather_parts(got_h[axis][0].astype(F32), got_h[axis])

    phase("drain")
    await_sent(rows.at[pl.ds(0, 3)], ag_s)
    await_sent(out_buf.at[pl.ds(0, n_dp - 1)], fe_s)
    await_sent(rt_others, rt_s)
    await_sent(score_buf.at[pl.ds(0, n_mp - 1)], sc_s)
    await_sent(back_buf.at[pl.ds(0, n_dp - 1)], ba_s)
    for axis in range(2):

        @pl.when(core == home[axis])
        def _():
            await_sent(grads[axis].at[pl.ds(0, 6 * ql)], gr_s.at[axis])
            await_sent(part_h[axis].at[pl.ds(0, 7)], hg_s.at[axis])

        @pl.when(core != home[axis])
        def _():
            await_sent(grads[axis].at[pl.ds(0, 8 * ql)], gr_s.at[axis])

    await_sent(part_q.at[pl.ds(1, n_mp - 1)], pq_s)
    await_sent(part_d.at[pl.ds(1, n_mp - 1)], pd_s)
    phase(None)


def hand_out(a, b, c, out_a, out_b, out_c, sem):
    copies = [
        pltpu.make_async_copy(src, dst, sem.at[i])
        for i, (src, dst) in enumerate(((c, out_c), (a, out_a), (b, out_b)))
    ]
    for copy in copies:
        copy.start()
    for copy in copies:
        copy.wait()


def on_device(query_rows, doc_rows, head, logit_scale, loss_grad, shortlist, send_rows):
    ql, cols = query_rows.shape
    dma = pltpu.SemaphoreType.DMA
    one = dma(())
    hbm = pl.BlockSpec(memory_space=pltpu.HBM)
    vmem = pl.BlockSpec(memory_space=pltpu.VMEM)
    operands = (logit_scale, loss_grad.T, shortlist, send_rows, query_rows, doc_rows, head)
    shapes = (
        jax.ShapeDtypeStruct((ql, cols), BF16),
        jax.ShapeDtypeStruct((ql, cols), BF16),
        jax.ShapeDtypeStruct((80, cols), F32),
    )
    results = pl.pallas_call(
        kernel,
        out_shape=shapes,
        in_specs=[hbm] * 7,
        out_specs=(vmem, vmem, vmem),
        scratch_shapes=[
            pltpu.SMEM((NW,), F32),
            pltpu.VMEM((NW, ql), F32),
            pltpu.VMEM((ql, 128), jnp.int32),
            pltpu.VMEM((1, 128), jnp.int32),
            pltpu.VMEM((4, 2 * ql, cols), BF16),
            pltpu.VMEM((4 * cols, cols), BF16),
            pltpu.VMEM((4, 4, 2, 80, 128), BF16),
            pltpu.VMEM((4, 2, 80, 1024), BF16),
            pltpu.VMEM((1024, 384), BF16),
            pltpu.VMEM((1024, 256), BF16),
            pltpu.VMEM((32, 4, cols), BF16),
            pltpu.VMEM((32, 4, cols), BF16),
            pltpu.VMEM((32, 4, cols), BF16),
            pltpu.VMEM((32, 4, cols), BF16),
            pltpu.VMEM((4, ql + 8, 128), F32),
            pltpu.VMEM((4, ql, cols), BF16),
            pltpu.VMEM((4, ql, cols), BF16),
            pltpu.VMEM((4, ql, cols), BF16),
            pltpu.VMEM((4, ql, cols), BF16),
            pltpu.VMEM((80, 384), F32),
            pltpu.VMEM((80, 256), F32),
            pltpu.VMEM((8, 80, 384), BF16),
            pltpu.VMEM((8, 80, 256), BF16),
            pltpu.VMEM((4, 80, 384), BF16),
            pltpu.VMEM((4, 80, 256), BF16),
            dma((10,)), one, dma((16,)), one, one, one, one, one, one, one, one,
            dma((2,)), one, one, one, one, one, dma((2,)), dma((2,)),
            pltpu.SemaphoreType.REGULAR((4,)),
        ],
        compiler_params=pltpu.CompilerParams(
            collective_id=0, has_side_effects=True, vmem_limit_bytes=48 * 1024 * 1024
        ),
    )(*[pltpu.with_memory_space_constraint(a, pltpu.HBM) for a in operands])
    anywhere = pl.BlockSpec(memory_space=pl.ANY)
    return pl.pallas_call(
        hand_out,
        out_shape=shapes,
        in_specs=[anywhere] * 3,
        out_specs=(anywhere,) * 3,
        scratch_shapes=[dma((3,))],
        compiler_params=pltpu.CompilerParams(vmem_limit_bytes=1024 * 1024),
    )(*results)


def solution(mesh):
    placed = (
        P("dp", "mp"),
        P("dp", "mp"),
        P(None, "mp"),
        P(),
        P("dp", None),
        P("dp", None),
        P("dp", None),
    )
    return jax.shard_map(
        on_device,
        mesh=mesh,
        in_specs=placed,
        out_specs=(P("dp", "mp"), P("dp", "mp"), P("dp", "mp")),
        check_vma=False,
    )
```

```python
import functools
import math

import jax
import jax.numpy as jnp
from jax import lax
from jax.experimental import pallas as pl
from jax.experimental.pallas import tpu as pltpu
from jax.sharding import PartitionSpec as P

NW = 7
LOCAL = 5
MESH = pl.DeviceIdType.MESH
F32 = jnp.float32
BF16 = jnp.bfloat16


def remote(src, dst, send_sem, recv_sem, device):
    return pltpu.make_async_remote_copy(
        src_ref=src,
        dst_ref=dst,
        send_sem=send_sem,
        recv_sem=recv_sem,
        device_id=device,
        device_id_type=MESH,
    )


class Phases:
    def __init__(self):
        self.open = None

    def __call__(self, name):
        if self.open is not None:
            self.open.__exit__(None, None, None)
        self.open = jax.named_scope(name) if name else None
        if self.open is not None:
            self.open.__enter__()


def contract(a, b, da, db):
    return lax.dot_general(a, b, (((da,), (db,)), ((), ())), preferred_element_type=F32)


def softmax_terms(score, pos, count, scale, weight):
    logit = jnp.where(count > 0.0, score * scale, -jnp.inf)
    pos_logit = pos * scale
    highest = jnp.maximum(jnp.max(logit, axis=1, keepdims=True), pos_logit)
    neg_exp = count * jnp.exp(logit - highest)
    pos_exp = jnp.exp(pos_logit - highest)
    denominator = jnp.sum(neg_exp, axis=1, keepdims=True) + pos_exp
    row_weight = weight * scale
    return neg_exp * (row_weight / denominator), row_weight * (pos_exp / denominator - 1.0)


def kernel(
    scale_hbm, loss_hbm, short_hbm, send_hbm, q_hbm, d_hbm, head_hbm,
    qg_ref, dg_ref, hg_ref,
    scale_ref, loss_ref, short_ref, send_ref, rows, head, rows_t, rt_buf, grads_0, grads_1,
    out_buf, fetched, back_buf, returned,
    score_buf, part_q, got_q, part_d, got_d,
    full_0, full_1, part_0, part_1, got_0, got_1,
    load_sem, ag_s, ag_r, fe_s, fe_r, sc_s, sc_r, rt_s, rt_r, ba_s, ba_r,
    gr_s, gr_r, pq_s, pq_r, pd_s, pd_r, hg_s, hg_r, word,
):
    n_dp, n_mp, ql, cols = 32, 4, 64, 640
    group = 8
    slots = 128
    block = 4
    hrows = 80
    cuts = (0, 384, cols)
    grads, full_h, part_h, got_h = (
        (grads_0, grads_1), (full_0, full_1), (part_0, part_1), (got_0, got_1)
    )
    me = lax.axis_index("dp")
    my = lax.axis_index("mp")
    x = me // group
    g = me % group
    z = g // 2
    feature_total = n_mp * cols
    bounds = [0] + [feature_total // 2 ** (NW - 1 - w) for w in range(NW)]

    def row_block(m):
        return pl.ds(pl.multiple_of(m * cols, cols), cols)

    phase = Phases()
    phase("loads")
    load_q = pltpu.make_async_copy(q_hbm, rows.at[my, pl.ds(0, ql)], load_sem.at[0])
    load_d = pltpu.make_async_copy(d_hbm, rows.at[my, pl.ds(ql, ql)], load_sem.at[1])
    load_short = pltpu.make_async_copy(short_hbm, short_ref, load_sem.at[6])
    load_send = pltpu.make_async_copy(send_hbm, send_ref, load_sem.at[7])
    load_loss = pltpu.make_async_copy(loss_hbm, loss_ref, load_sem.at[8])
    load_scale = pltpu.make_async_copy(scale_hbm, scale_ref, load_sem.at[9])
    load_d.start()
    load_q.start()
    load_short.start()
    load_send.start()
    load_loss.start()
    load_scale.start()
    order = (0, 1, 3, 2)
    load_h = []
    for k in order:
        src = (my + n_mp - k) % n_mp
        copy = pltpu.make_async_copy(
            head_hbm.at[row_block(src)], head.at[row_block(src)], load_sem.at[2 + k]
        )
        copy.start()
        load_h.append(copy)

    phase("greet")
    right, left = (my + 1) % n_mp, (my + n_mp - 1) % n_mp
    far = (my + 2) % n_mp
    core = me % 2
    partner = me + 1 - 2 * core
    x_near = ((me + group) % n_dp, (me + n_dp - group) % n_dp)
    z_near = (x * group + (g + 2) % group, x * group + (g + 6) % group)
    barrier = pltpu.get_barrier_semaphore()
    near = [(me, right), (me, left), (me, far), (partner, my)]
    near += [(peer, my) for peer in x_near + z_near]
    for device in near:
        pl.semaphore_signal(barrier, inc=1, device_id=device, device_id_type=MESH)

    def await_sent(ref, sem):
        remote(ref, ref, sem, sem, (me, my)).wait_send()

    def await_got(ref, sem):
        remote(ref, ref, sem, sem, (me, my)).wait_recv()

    steps = [(i, j, k) for i in (2, 1, 3, 0) for j in (2, 1, 3, 0) for k in (0, 1)]
    steps.sort(key=lambda d: -(min(d[0], 4 - d[0]) + min(d[1], 4 - d[1])))
    others = [
        ((x + i) % 4 * group + (z + j) % 4 * 2 + (core if k == 0 else 1 - core))
        for i, j, k in steps
        if (i, j, k) != (0, 0, 0)
    ]

    def tell(step, peers):
        for peer in peers:
            pl.semaphore_signal(
                word.at[step], inc=1, device_id=(peer, my), device_id_type=MESH
            )

    def hear(step, count):
        pl.semaphore_wait(word.at[step], count)

    load_d.wait()
    pl.semaphore_wait(barrier, len(near))

    half, quarter = ql // 2, ql // 4
    row_pieces = (
        (0, half, far),
        (half, quarter, right),
        (half + quarter, quarter, right),
        (0, half, right),
        (half + quarter, quarter, left),
        (0, half + quarter, left),
        (half, quarter, right),
        (half + quarter, quarter, left),
    )

    def row_copy(part, slot, src):
        first, count, peer = row_pieces[slot]
        at = pl.ds((1 - part) * ql + first, count)
        slot = part * 8 + slot
        return remote(
            rows.at[src, at], rows.at[src, at], ag_s, ag_r.at[slot], (me, peer)
        )

    def rows_start(part):
        for slot in (1, 4, 0, 2, 3, 5):
            row_copy(part, slot, my).start()

    def rows_relay(part):
        for slot, src in ((1, left), (4, right)):
            row_copy(part, slot, src).wait_recv()
            row_copy(part, 6 if slot == 1 else 7, src).start()

    def rows_right(part):
        row_copy(part, 5, right).wait_recv()
        return product_of(part, right)

    def rows_left(part):
        for slot in (2, 3):
            row_copy(part, slot, left).wait_recv()
        return product_of(part, left)

    def rows_far(part):
        for slot in (0, 6, 7):
            row_copy(part, slot, far).wait_recv()
        return product_of(part, far)

    def product_of(part, src):
        at = (1 - part) * ql
        return jnp.dot(
            rows[src, at : at + ql, :], head[row_block(src), :], preferred_element_type=F32
        )

    home = (1, 0)
    chips = (z, x)
    spots = (x, z)

    bands = (((0, 384),), ((0, 256),))

    def gatherer(axis, pos):
        return x * group + pos * 2 + home[0] if axis == 0 else pos * group + z * 2 + home[1]

    def reducer(axis, pos, c):
        return pos * group + z * 2 + c if axis == 0 else x * group + pos * 2 + c

    def place(k):
        return pl.multiple_of(k * 2 * slots + core * slots, slots)

    def turned(axis, pos):
        return rows_t.at[:, pos] if axis == 0 else rows_t.at[pos]

    def turn_rows(m):
        rows_t[m] = rows[m].T.reshape(n_mp, 2, hrows, slots)

    def turn_start(axes):
        for axis in axes:
            own = pl.ds(place(0), slots)
            for k in (2, 1, 3):
                pos = (chips[axis] + k) % n_mp
                remote(
                    turned(axis, pos), rt_buf.at[:, :, :, pl.ds(place(k), slots)], rt_s, rt_r,
                    (gatherer(axis, pos), my),
                ).start()

            @pl.when(core == home[axis])
            def _():
                rt_buf[:, :, :, own] = turned(axis, chips[axis])[...]

            @pl.when(core != home[axis])
            def _():
                remote(
                    turned(axis, chips[axis]), rt_buf.at[:, :, :, own], rt_s, rt_r, (partner, my)
                ).start()

    rt_others = rt_buf.at[:, :, :, pl.ds(0, (group - 1) * slots)]

    phase("rows_d")
    rows_start(0)
    tell(0, x_near)
    load_h[0].wait()
    acc = product_of(0, my)
    load_send.wait()
    pick = jnp.where(
        lax.broadcasted_iota(jnp.int32, (ql, slots), 0) == send_ref[...], 1.0, 0.0
    ).astype(BF16)

    for copy in load_h[1:]:
        copy.wait()
    hear(0, 2)
    tell(1, z_near)
    phase("relay_d")
    rows_relay(0)
    hear(1, 2)
    tell(2, z_near)
    phase("right_d")
    acc = acc + rows_right(0)
    load_q.wait()
    rows_start(1)
    hear(2, 2)
    tell(3, (partner,))
    phase("left_d")
    acc = acc + rows_left(0)
    phase("far_d")
    acc = acc + rows_far(0)
    hear(3, 1)
    phase("pick")
    dp = acc.astype(BF16)

    picked = contract(pick, dp, 0, 0).astype(BF16)
    out_buf[...] = picked.reshape(n_dp, block, cols)

    phase("fetch")
    for peer in others:
        remote(out_buf.at[peer], fetched.at[me], fe_s, fe_r, (peer, my)).start()
    fetched[me] = out_buf[me]

    phase("relay_q")
    rows_relay(1)
    phase("count")
    load_loss.wait()
    load_scale.wait()
    weight = loss_ref[...].T
    load_short.wait()
    short = short_ref[...]
    lane = lax.broadcasted_iota(jnp.int32, (ql, slots), 1)

    count = jnp.zeros((ql, slots), F32)
    for k in range(slots):
        count = count + jnp.where((short if k == 0 else pltpu.roll(short, k, 1)) == lane, 1.0, 0.0)
    phase("rows_q")
    acc = product_of(1, my)
    turn_rows(my)
    acc = acc + rows_right(1)
    turn_rows(right)
    acc = acc + rows_left(1)
    turn_rows(left)
    acc = acc + rows_far(1)
    qp = acc.astype(BF16)

    phase("turn0")
    turn_rows(far)
    turn_start((1, 0))
    phase("mask")
    col = lax.broadcasted_iota(jnp.int32, (1, cols), 1)
    seg_col = [
        jnp.where((col >= bounds[s]) & (col < bounds[s + 1]), 1.0, 0.0) for s in range(LOCAL)
    ]
    product = qp.astype(F32) * dp.astype(F32)
    pos_whole = jnp.sum(product, axis=1, keepdims=True)
    diag = lax.broadcasted_iota(jnp.int32, (ql, slots), 0) == lane
    pos_row = jnp.sum(
        jnp.where(diag, jnp.broadcast_to(pos_whole, (ql, slots)), 0.0), axis=0, keepdims=True
    )
    score_buf[my, ql : ql + 8, :] = jnp.broadcast_to(pos_row, (8, slots))

    phase("fetch_wait")
    await_got(fetched.at[pl.ds(0, n_dp - 1)], fe_r)
    phase("score")
    docs = fetched[...].reshape(slots, cols)
    whole = contract(qp, docs, 1, 1)
    score_buf[my, 0:ql, :] = whole
    for peer in (far, right, left):
        remote(score_buf.at[my], score_buf.at[my], sc_s, sc_r, (me, peer)).start()

    phase("narrow")
    def width(w, score, pos):
        scale = scale_ref[w] * (1.0 / math.sqrt(bounds[w + 1]))
        return softmax_terms(score, pos, count, scale, weight[:, w : w + 1])

    q_seg = jnp.concatenate([qp * m.astype(BF16) for m in seg_col], axis=0)
    pos_prefix = [
        jnp.sum(
            product * jnp.where(col < bounds[s + 1], 1.0, 0.0), axis=1, keepdims=True
        )
        for s in range(LOCAL - 1)
    ] + [pos_whole]
    pieces = contract(q_seg[: 4 * ql], docs, 1, 1)
    scores = []
    for s in range(LOCAL - 1):
        piece = pieces[s * ql : (s + 1) * ql]
        scores.append(piece if s == 0 else scores[-1] + piece)
    scores.append(whole)
    narrow = [width(w, scores[w], pos_prefix[w]) for w in range(LOCAL)]
    for s in reversed(range(LOCAL - 1)):
        narrow[s] = tuple(a + b for a, b in zip(narrow[s], narrow[s + 1]))
    narrow = [tuple(jnp.where(my == 0, a, 0.0) for a in terms) for terms in narrow]
    doc_seg = [docs * m.astype(BF16) for m in seg_col]
    wide_at = 256
    docs_low = jnp.concatenate([m[:, :wide_at] for m in doc_seg[:4]], axis=0)
    docs_high = jnp.concatenate([m[:, wide_at:] for m in doc_seg[3:]], axis=0)

    phase("score_wait")
    await_got(score_buf.at[pl.ds(0, n_mp - 1)], sc_r)
    phase("wide")
    parts = [score_buf[m, 0:ql, :] for m in range(n_mp)]
    pos_rows = [score_buf[m, ql : ql + 8, :] for m in range(n_mp)]
    pos_row5 = pos_rows[0] + pos_rows[1]
    pos5, pos6 = [
        jnp.sum(
            jnp.where(diag, jnp.concatenate([row] * 8, axis=0), 0.0), axis=1, keepdims=True
        )
        for row in (pos_row5, pos_row5 + (pos_rows[2] + pos_rows[3]))
    ]
    score5 = parts[0] + parts[1]
    neg5, posg5 = width(5, score5, pos5)
    neg6, posg6 = width(6, score5 + (parts[2] + parts[3]), pos6)
    run_neg = neg6 + jnp.where(my <= 1, neg5, 0.0)
    run_pos = posg6 + jnp.where(my <= 1, posg5, 0.0)
    coeff = [(run_neg + narrow[s][0]).astype(BF16) for s in range(LOCAL)]

    phase("by_slot")
    by_slot = jnp.concatenate(
        [
            contract(jnp.concatenate(coeff[:4], axis=0), q_seg[: 4 * ql, :wide_at], 0, 0),
            contract(jnp.concatenate(coeff[3:], axis=0), q_seg[3 * ql :, wide_at:], 0, 0),
        ],
        axis=1,
    ).astype(BF16)
    back_buf[...] = by_slot.reshape(n_dp, block, cols)

    for peer in others:
        remote(back_buf.at[peer], returned.at[me], ba_s, ba_r, (peer, my)).start()
    returned[me] = back_buf[me]

    phase("grad_q")
    pos_cols = (run_pos + narrow[0][1]) * seg_col[0]
    for s in range(1, LOCAL):
        pos_cols = pos_cols + (run_pos + narrow[s][1]) * seg_col[s]
    query_back = jnp.concatenate(
        [
            jnp.dot(jnp.concatenate(coeff[:4], axis=1), docs_low, preferred_element_type=F32),
            jnp.dot(jnp.concatenate(coeff[3:], axis=1), docs_high, preferred_element_type=F32),
        ],
        axis=1,
    )
    grad_q = (query_back + pos_cols * dp.astype(F32)).astype(BF16)

    def spread(part, grad):
        for axis in range(2):
            at = pl.ds(pl.multiple_of(place(0) + part * ql, ql), ql)
            grads[axis][at, :] = grad[:, cuts[axis] : cuts[axis + 1]]
        for band in range(len(bands[0])):
            for k in (2, 1, 3, 0):
                for axis in range(2):
                    columns = slice(*bands[axis][band])
                    own = pl.ds(pl.multiple_of(place(0) + part * ql, ql), ql)
                    there = pl.ds(pl.multiple_of(place(k) + part * ql, ql), ql)
                    src, dst = grads[axis].at[own, columns], grads[axis].at[there, columns]
                    if k:
                        device = gatherer(axis, (chips[axis] + k) % n_mp)
                        remote(src, dst, gr_s.at[axis], gr_r, (device, my)).start()
                    else:

                        @pl.when(core != home[axis])
                        def _():
                            remote(src, dst, gr_s.at[axis], gr_r, (partner, my)).start()

    def share(grad, part, got, send_sem, recv_sem):
        for k in (2, 1, 3):
            peer = (my + k) % n_mp
            part[k] = contract(grad, head[row_block(peer), :], 1, 1).astype(BF16)
            remote(part.at[k], got.at[k], send_sem, recv_sem, (me, peer)).start()
        return contract(grad, head[row_block(my), :], 1, 1)

    def gather_parts(own, got):
        for k in (1, 3, 2):
            own = own + got[k].astype(F32)
        return own

    phase("share_q")
    own_q = share(grad_q, part_q, got_q, pq_s, pq_r)

    phase("spread_q")
    spread(0, grad_q)
    phase("back_wait")
    await_got(returned.at[pl.ds(0, n_dp - 1)], ba_r)
    phase("grad_d")
    doc_back = jnp.dot(pick, returned[...].reshape(slots, cols), preferred_element_type=F32)
    grad_d = (pos_cols * qp.astype(F32) + doc_back).astype(BF16)
    spread(1, grad_d)
    phase("share_d")
    own_d = share(grad_d, part_d, got_d, pd_s, pd_r)
    phase("rt_wait")
    await_got(rt_others, rt_r)
    phase(None)

    def head_part(axis):
        with jax.named_scope("gather_h"):
            await_got(grads[axis].at[pl.ds(0, 7 * slots)], gr_r)
        for n in (2, 1, 3, 0):
            pos = (spots[axis] + n) % n_mp
            with jax.named_scope("head%d" % n):
                block = jnp.dot(
                    rt_buf[pos].reshape(2 * hrows, n_mp * 2 * slots), grads[axis][...],
                    preferred_element_type=F32,
                )
                part_h[axis][pl.ds(pos * 2, 2)] = block.astype(BF16).reshape(2, hrows, -1)
                if n == 0:
                    full_h[axis][...] = block[home[axis] * hrows : (home[axis] + 1) * hrows]
                    remote(
                        part_h[axis].at[pos * 2 + 1 - home[axis]], got_h[axis].at[0],
                        hg_s.at[axis], hg_r.at[axis], (partner, my),
                    ).start()
                for i in range(2 if n else 0):
                    remote(
                        part_h[axis].at[pos * 2 + i], got_h[axis].at[n],
                        hg_s.at[axis], hg_r.at[axis], (reducer(axis, pos, i), my),
                    ).start()

    for axis in range(2):
        pl.when(core == home[axis])(functools.partial(head_part, axis))
    phase("query_out")
    await_got(got_q.at[pl.ds(1, n_mp - 1)], pq_r)
    qg_ref[...] = gather_parts(own_q, got_q).astype(BF16)

    phase("doc_out")
    await_got(got_d.at[pl.ds(1, n_mp - 1)], pd_r)
    dg_ref[...] = gather_parts(own_d, got_d).astype(BF16)
    phase("head_out")
    for axis in range(2):
        columns = slice(cuts[axis], cuts[axis + 1])

        @pl.when(core == home[axis])
        def _():
            await_got(got_h[axis].at[pl.ds(1, n_mp - 1)], hg_r.at[axis])
            hg_ref[:, columns] = gather_parts(full_h[axis][...], got_h[axis])

        @pl.when(core != home[axis])
        def _():
            await_got(got_h[axis], hg_r.at[axis])
            hg_ref[:, columns] = gather_parts(got_h[axis][0].astype(F32), got_h[axis])

    phase("drain")
    await_sent(rows.at[pl.ds(0, 3)], ag_s)
    await_sent(out_buf.at[pl.ds(0, n_dp - 1)], fe_s)
    await_sent(rt_others, rt_s)
    await_sent(score_buf.at[pl.ds(0, n_mp - 1)], sc_s)
    await_sent(back_buf.at[pl.ds(0, n_dp - 1)], ba_s)
    for axis in range(2):

        @pl.when(core == home[axis])
        def _():
            await_sent(grads[axis].at[pl.ds(0, 6 * ql)], gr_s.at[axis])
            await_sent(part_h[axis].at[pl.ds(0, 7)], hg_s.at[axis])

        @pl.when(core != home[axis])
        def _():
            await_sent(grads[axis].at[pl.ds(0, 8 * ql)], gr_s.at[axis])

    await_sent(part_q.at[pl.ds(1, n_mp - 1)], pq_s)
    await_sent(part_d.at[pl.ds(1, n_mp - 1)], pd_s)
    phase(None)


def hand_out(a, b, c, out_a, out_b, out_c, sem):
    copies = [
        pltpu.make_async_copy(src, dst, sem.at[i])
        for i, (src, dst) in enumerate(((c, out_c), (a, out_a), (b, out_b)))
    ]
    for copy in copies:
        copy.start()
    for copy in copies:
        copy.wait()


def on_device(query_rows, doc_rows, head, logit_scale, loss_grad, shortlist, send_rows):
    ql, cols = query_rows.shape
    dma = pltpu.SemaphoreType.DMA
    one = dma(())
    hbm = pl.BlockSpec(memory_space=pltpu.HBM)
    vmem = pl.BlockSpec(memory_space=pltpu.VMEM)
    operands = (logit_scale, loss_grad.T, shortlist, send_rows, query_rows, doc_rows, head)
    shapes = (
        jax.ShapeDtypeStruct((ql, cols), BF16),
        jax.ShapeDtypeStruct((ql, cols), BF16),
        jax.ShapeDtypeStruct((80, cols), F32),
    )
    results = pl.pallas_call(
        kernel,
        out_shape=shapes,
        in_specs=[hbm] * 7,
        out_specs=(vmem, vmem, vmem),
        scratch_shapes=[
            pltpu.SMEM((NW,), F32),
            pltpu.VMEM((NW, ql), F32),
            pltpu.VMEM((ql, 128), jnp.int32),
            pltpu.VMEM((1, 128), jnp.int32),
            pltpu.VMEM((4, 2 * ql, cols), BF16),
            pltpu.VMEM((4 * cols, cols), BF16),
            pltpu.VMEM((4, 4, 2, 80, 128), BF16),
            pltpu.VMEM((4, 2, 80, 1024), BF16),
            pltpu.VMEM((1024, 384), BF16),
            pltpu.VMEM((1024, 256), BF16),
            pltpu.VMEM((32, 4, cols), BF16),
            pltpu.VMEM((32, 4, cols), BF16),
            pltpu.VMEM((32, 4, cols), BF16),
            pltpu.VMEM((32, 4, cols), BF16),
            pltpu.VMEM((4, ql + 8, 128), F32),
            pltpu.VMEM((4, ql, cols), BF16),
            pltpu.VMEM((4, ql, cols), BF16),
            pltpu.VMEM((4, ql, cols), BF16),
            pltpu.VMEM((4, ql, cols), BF16),
            pltpu.VMEM((80, 384), F32),
            pltpu.VMEM((80, 256), F32),
            pltpu.VMEM((8, 80, 384), BF16),
            pltpu.VMEM((8, 80, 256), BF16),
            pltpu.VMEM((4, 80, 384), BF16),
            pltpu.VMEM((4, 80, 256), BF16),
            dma((10,)), one, dma((16,)), one, one, one, one, one, one, one, one,
            dma((2,)), one, one, one, one, one, dma((2,)), dma((2,)),
            pltpu.SemaphoreType.REGULAR((4,)),
        ],
        compiler_params=pltpu.CompilerParams(
            collective_id=0, has_side_effects=True, vmem_limit_bytes=48 * 1024 * 1024
        ),
    )(*[pltpu.with_memory_space_constraint(a, pltpu.HBM) for a in operands])
    anywhere = pl.BlockSpec(memory_space=pl.ANY)
    return pl.pallas_call(
        hand_out,
        out_shape=shapes,
        in_specs=[anywhere] * 3,
        out_specs=(anywhere,) * 3,
        scratch_shapes=[dma((3,))],
        compiler_params=pltpu.CompilerParams(vmem_limit_bytes=1024 * 1024),
    )(*results)


def solution(mesh):
    placed = (
        P("dp", "mp"),
        P("dp", "mp"),
        P(None, "mp"),
        P(),
        P("dp", None),
        P("dp", None),
        P("dp", None),
    )
    return jax.shard_map(
        on_device,
        mesh=mesh,
        in_specs=placed,
        out_specs=(P("dp", "mp"), P("dp", "mp"), P("dp", "mp")),
        check_vma=False,
    )
```

```python
import functools
import math

import jax
import jax.numpy as jnp
from jax import lax
from jax.experimental import pallas as pl
from jax.experimental.pallas import tpu as pltpu
from jax.sharding import PartitionSpec as P

NW = 7
LOCAL = 5
MESH = pl.DeviceIdType.MESH
F32 = jnp.float32
BF16 = jnp.bfloat16


def remote(src, dst, send_sem, recv_sem, device):
    return pltpu.make_async_remote_copy(
        src_ref=src,
        dst_ref=dst,
        send_sem=send_sem,
        recv_sem=recv_sem,
        device_id=device,
        device_id_type=MESH,
    )


class Phases:
    def __init__(self):
        self.open = None

    def __call__(self, name):
        if self.open is not None:
            self.open.__exit__(None, None, None)
        self.open = jax.named_scope(name) if name else None
        if self.open is not None:
            self.open.__enter__()


def contract(a, b, da, db):
    return lax.dot_general(a, b, (((da,), (db,)), ((), ())), preferred_element_type=F32)


def softmax_terms(score, pos, count, scale, weight):
    logit = jnp.where(count > 0.0, score * scale, -jnp.inf)
    pos_logit = pos * scale
    highest = jnp.maximum(jnp.max(logit, axis=1, keepdims=True), pos_logit)
    neg_exp = count * jnp.exp(logit - highest)
    pos_exp = jnp.exp(pos_logit - highest)
    denominator = jnp.sum(neg_exp, axis=1, keepdims=True) + pos_exp
    row_weight = weight * scale
    return neg_exp * (row_weight / denominator), row_weight * (pos_exp / denominator - 1.0)


def kernel(
    scale_hbm, loss_hbm, short_hbm, send_hbm, q_hbm, d_hbm, head_hbm,
    qg_ref, dg_ref, hg_ref,
    scale_ref, loss_ref, short_ref, send_ref, rows, head, rows_t, rt_buf, grads_0, grads_1,
    out_buf, fetched, back_buf, returned,
    score_buf, part_q, got_q, part_d, got_d,
    own_0, own_1, full_0, full_1, part_0, part_1, got_0, got_1,
    load_sem, ag_s, ag_r, fe_s, fe_r, sc_s, sc_r, rt_s, rt_r, ba_s, ba_r,
    gr_s, gr_r, pq_s, pq_r, pd_s, pd_r, hg_s, hg_r, word,
):
    n_dp, n_mp, ql, cols = 32, 4, 64, 640
    group = 8
    slots = 128
    block = 4
    hrows = 80
    cuts = (0, 384, cols)
    grads, own_h, full_h, part_h, got_h = (
        (grads_0, grads_1), (own_0, own_1), (full_0, full_1), (part_0, part_1), (got_0, got_1)
    )
    me = lax.axis_index("dp")
    my = lax.axis_index("mp")
    x = me // group
    g = me % group
    z = g // 2
    feature_total = n_mp * cols
    bounds = [0] + [feature_total // 2 ** (NW - 1 - w) for w in range(NW)]

    def row_block(m):
        return pl.ds(pl.multiple_of(m * cols, cols), cols)

    phase = Phases()
    phase("loads")
    load_q = pltpu.make_async_copy(q_hbm, rows.at[my, pl.ds(0, ql)], load_sem.at[0])
    load_d = pltpu.make_async_copy(d_hbm, rows.at[my, pl.ds(ql, ql)], load_sem.at[1])
    load_short = pltpu.make_async_copy(short_hbm, short_ref, load_sem.at[6])
    load_send = pltpu.make_async_copy(send_hbm, send_ref, load_sem.at[7])
    load_loss = pltpu.make_async_copy(loss_hbm, loss_ref, load_sem.at[8])
    load_scale = pltpu.make_async_copy(scale_hbm, scale_ref, load_sem.at[9])
    load_d.start()
    load_q.start()
    load_short.start()
    load_send.start()
    load_loss.start()
    load_scale.start()
    order = (0, 1, 3, 2)
    load_h = []
    for k in order:
        src = (my + n_mp - k) % n_mp
        copy = pltpu.make_async_copy(
            head_hbm.at[row_block(src)], head.at[row_block(src)], load_sem.at[2 + k]
        )
        copy.start()
        load_h.append(copy)

    phase("greet")
    right, left = (my + 1) % n_mp, (my + n_mp - 1) % n_mp
    far = (my + 2) % n_mp
    core = me % 2
    partner = me + 1 - 2 * core
    x_near = ((me + group) % n_dp, (me + n_dp - group) % n_dp)
    z_near = (x * group + (g + 2) % group, x * group + (g + 6) % group)
    barrier = pltpu.get_barrier_semaphore()
    near = [(me, right), (me, left), (me, far), (partner, my)]
    near += [(peer, my) for peer in x_near + z_near]
    for device in near:
        pl.semaphore_signal(barrier, inc=1, device_id=device, device_id_type=MESH)

    def await_sent(ref, sem):
        remote(ref, ref, sem, sem, (me, my)).wait_send()

    def await_got(ref, sem):
        remote(ref, ref, sem, sem, (me, my)).wait_recv()

    steps = [(i, j, k) for i in (2, 1, 3, 0) for j in (2, 1, 3, 0) for k in (0, 1)]
    steps.sort(key=lambda d: -(min(d[0], 4 - d[0]) + min(d[1], 4 - d[1])))
    others = [
        ((x + i) % 4 * group + (z + j) % 4 * 2 + (core if k == 0 else 1 - core))
        for i, j, k in steps
        if (i, j, k) != (0, 0, 0)
    ]

    def tell(step, peers):
        for peer in peers:
            pl.semaphore_signal(
                word.at[step], inc=1, device_id=(peer, my), device_id_type=MESH
            )

    def hear(step, count):
        pl.semaphore_wait(word.at[step], count)

    load_d.wait()
    pl.semaphore_wait(barrier, len(near))

    half, quarter = ql // 2, ql // 4
    row_pieces = (
        (0, half, far),
        (half, quarter, right),
        (half + quarter, quarter, right),
        (0, half, right),
        (half + quarter, quarter, left),
        (0, half + quarter, left),
        (half, quarter, right),
        (half + quarter, quarter, left),
    )

    def row_copy(part, slot, src):
        first, count, peer = row_pieces[slot]
        at = pl.ds((1 - part) * ql + first, count)
        slot = part * 5 + (0, 1, 2, 2, 3, 4, 0, 0)[slot]
        return remote(
            rows.at[src, at], rows.at[src, at], ag_s, ag_r.at[slot], (me, peer)
        )

    def rows_start(part):
        for slot in (1, 4, 0, 2, 3, 5):
            row_copy(part, slot, my).start()

    def rows_relay(part):
        for slot, src in ((1, left), (4, right)):
            row_copy(part, slot, src).wait_recv()
            row_copy(part, 6 if slot == 1 else 7, src).start()

    def rows_right(part):
        row_copy(part, 5, right).wait_recv()
        return product_of(part, right)

    def rows_left(part):
        await_got(rows.at[left, pl.ds(0, half + quarter)], ag_r.at[part * 5 + 2])
        return product_of(part, left)

    def rows_far(part):
        await_got(rows.at[far, pl.ds(0, ql)], ag_r.at[part * 5])
        return product_of(part, far)

    def product_of(part, src):
        at = (1 - part) * ql
        return jnp.dot(
            rows[src, at : at + ql, :], head[row_block(src), :], preferred_element_type=F32
        )

    home = (1, 0)
    chips = (z, x)
    spots = (x, z)

    bands = (((0, 384),), ((0, 256),))

    def gatherer(axis, pos):
        return x * group + pos * 2 + home[0] if axis == 0 else pos * group + z * 2 + home[1]

    def reducer(axis, pos, c):
        return pos * group + z * 2 + c if axis == 0 else x * group + pos * 2 + c

    def place(k):
        return pl.multiple_of(k * 2 * slots + core * slots, slots)

    def turned(axis, pos):
        return rows_t.at[:, pos] if axis == 0 else rows_t.at[pos]

    def turn_rows(m):
        rows_t[m] = rows[m].T.reshape(n_mp, 2, hrows, slots)

    def turn_start(axes):
        for axis in axes:
            own = pl.ds(place(0), slots)
            for k in (2, 1, 3):
                pos = (chips[axis] + k) % n_mp
                remote(
                    turned(axis, pos), rt_buf.at[:, :, :, pl.ds(place(k), slots)], rt_s, rt_r,
                    (gatherer(axis, pos), my),
                ).start()

            @pl.when(core == home[axis])
            def _():
                rt_buf[:, :, :, own] = turned(axis, chips[axis])[...]

            @pl.when(core != home[axis])
            def _():
                remote(
                    turned(axis, chips[axis]), rt_buf.at[:, :, :, own], rt_s, rt_r, (partner, my)
                ).start()

    rt_others = rt_buf.at[:, :, :, pl.ds(0, (group - 1) * slots)]

    phase("rows_d")
    rows_start(0)
    tell(0, x_near)
    load_h[0].wait()
    acc = product_of(0, my)
    load_send.wait()
    pick = jnp.where(
        lax.broadcasted_iota(jnp.int32, (ql, slots), 0) == send_ref[...], 1.0, 0.0
    ).astype(BF16)

    for copy in load_h[1:]:
        copy.wait()
    hear(0, 2)
    tell(1, z_near)
    phase("relay_d")
    rows_relay(0)
    hear(1, 2)
    tell(2, z_near)
    phase("right_d")
    acc = acc + rows_right(0)
    load_q.wait()
    rows_start(1)
    hear(2, 2)
    tell(3, (partner,))
    phase("left_d")
    acc = acc + rows_left(0)
    phase("far_d")
    acc = acc + rows_far(0)
    hear(3, 1)
    phase("pick")
    dp = acc.astype(BF16)

    picked = contract(pick, dp, 0, 0).astype(BF16)
    out_buf[...] = picked.reshape(n_dp, block, cols)

    phase("fetch")
    for peer in others:
        remote(out_buf.at[peer], fetched.at[me], fe_s, fe_r, (peer, my)).start()
    fetched[me] = out_buf[me]

    phase("relay_q")
    rows_relay(1)
    phase("count")
    load_loss.wait()
    load_scale.wait()
    weight = loss_ref[...].T
    load_short.wait()
    short = short_ref[...]
    lane = lax.broadcasted_iota(jnp.int32, (ql, slots), 1)

    count = jnp.zeros((ql, slots), F32)
    for k in range(slots):
        count = count + jnp.where((short if k == 0 else pltpu.roll(short, k, 1)) == lane, 1.0, 0.0)
    phase("rows_q")
    acc = product_of(1, my)
    turn_rows(my)
    acc = acc + rows_right(1)
    turn_rows(right)
    acc = acc + rows_left(1)
    turn_rows(left)
    acc = acc + rows_far(1)
    qp = acc.astype(BF16)

    phase("turn0")
    turn_rows(far)
    turn_start((1, 0))
    phase("mask")
    col = lax.broadcasted_iota(jnp.int32, (1, cols), 1)
    seg_col = [
        jnp.where((col >= bounds[s]) & (col < bounds[s + 1]), 1.0, 0.0) for s in range(LOCAL)
    ]
    product = qp.astype(F32) * dp.astype(F32)
    pos_whole = jnp.sum(product, axis=1, keepdims=True)
    diag = lax.broadcasted_iota(jnp.int32, (ql, slots), 0) == lane
    pos_row = jnp.sum(
        jnp.where(diag, jnp.broadcast_to(pos_whole, (ql, slots)), 0.0), axis=0, keepdims=True
    )
    score_buf[my, ql : ql + 8, :] = jnp.broadcast_to(pos_row, (8, slots))

    phase("fetch_wait")
    await_got(fetched.at[pl.ds(0, n_dp - 1)], fe_r)
    phase("score")
    docs = fetched[...].reshape(slots, cols)
    whole = contract(qp, docs, 1, 1)
    score_buf[my, 0:ql, :] = whole
    for peer in (far, right, left):
        remote(score_buf.at[my], score_buf.at[my], sc_s, sc_r, (me, peer)).start()

    phase("narrow")
    def width(w, score, pos):
        scale = scale_ref[w] * (1.0 / math.sqrt(bounds[w + 1]))
        return softmax_terms(score, pos, count, scale, weight[:, w : w + 1])

    q_seg = jnp.concatenate([qp * m.astype(BF16) for m in seg_col], axis=0)
    pos_prefix = [
        jnp.sum(
            product * jnp.where(col < bounds[s + 1], 1.0, 0.0), axis=1, keepdims=True
        )
        for s in range(LOCAL - 1)
    ] + [pos_whole]
    pieces = contract(q_seg[: 4 * ql], docs, 1, 1)
    scores = []
    for s in range(LOCAL - 1):
        piece = pieces[s * ql : (s + 1) * ql]
        scores.append(piece if s == 0 else scores[-1] + piece)
    scores.append(whole)
    narrow = [width(w, scores[w], pos_prefix[w]) for w in range(LOCAL)]
    for s in reversed(range(LOCAL - 1)):
        narrow[s] = tuple(a + b for a, b in zip(narrow[s], narrow[s + 1]))
    narrow = [tuple(jnp.where(my == 0, a, 0.0) for a in terms) for terms in narrow]
    doc_seg = [docs * m.astype(BF16) for m in seg_col]
    wide_at = 256
    docs_low = jnp.concatenate([m[:, :wide_at] for m in doc_seg[:4]], axis=0)
    docs_high = jnp.concatenate([m[:, wide_at:] for m in doc_seg[3:]], axis=0)

    phase("score_wait")
    await_got(score_buf.at[pl.ds(0, n_mp - 1)], sc_r)
    phase("wide")
    parts = [score_buf[m, 0:ql, :] for m in range(n_mp)]
    pos_rows = [score_buf[m, ql : ql + 8, :] for m in range(n_mp)]
    pos_row5 = pos_rows[0] + pos_rows[1]
    pos5, pos6 = [
        jnp.sum(
            jnp.where(diag, jnp.concatenate([row] * 8, axis=0), 0.0), axis=1, keepdims=True
        )
        for row in (pos_row5, pos_row5 + (pos_rows[2] + pos_rows[3]))
    ]
    score5 = parts[0] + parts[1]
    neg5, posg5 = width(5, score5, pos5)
    neg6, posg6 = width(6, score5 + (parts[2] + parts[3]), pos6)
    run_neg = neg6 + jnp.where(my <= 1, neg5, 0.0)
    run_pos = posg6 + jnp.where(my <= 1, posg5, 0.0)
    coeff = [(run_neg + narrow[s][0]).astype(BF16) for s in range(LOCAL)]

    phase("by_slot")
    by_slot = jnp.concatenate(
        [
            contract(jnp.concatenate(coeff[:4], axis=0), q_seg[: 4 * ql, :wide_at], 0, 0),
            contract(jnp.concatenate(coeff[3:], axis=0), q_seg[3 * ql :, wide_at:], 0, 0),
        ],
        axis=1,
    ).astype(BF16)
    back_buf[...] = by_slot.reshape(n_dp, block, cols)

    for peer in others:
        remote(back_buf.at[peer], returned.at[me], ba_s, ba_r, (peer, my)).start()
    returned[me] = back_buf[me]

    phase("grad_q")
    pos_cols = (run_pos + narrow[0][1]) * seg_col[0]
    for s in range(1, LOCAL):
        pos_cols = pos_cols + (run_pos + narrow[s][1]) * seg_col[s]
    query_back = jnp.concatenate(
        [
            jnp.dot(jnp.concatenate(coeff[:4], axis=1), docs_low, preferred_element_type=F32),
            jnp.dot(jnp.concatenate(coeff[3:], axis=1), docs_high, preferred_element_type=F32),
        ],
        axis=1,
    )
    grad_q = (query_back + pos_cols * dp.astype(F32)).astype(BF16)

    def spread(part, grad):
        for axis in range(2):
            at = pl.ds(pl.multiple_of(place(0) + part * ql, ql), ql)
            grads[axis][at, :] = grad[:, cuts[axis] : cuts[axis + 1]]
        for band in range(len(bands[0])):
            for k in (2, 1, 3, 0):
                for axis in range(2):
                    columns = slice(*bands[axis][band])
                    own = pl.ds(pl.multiple_of(place(0) + part * ql, ql), ql)
                    there = pl.ds(pl.multiple_of(place(k) + part * ql, ql), ql)
                    src, dst = grads[axis].at[own, columns], grads[axis].at[there, columns]
                    if k:
                        device = gatherer(axis, (chips[axis] + k) % n_mp)
                        remote(src, dst, gr_s.at[axis], gr_r.at[1], (device, my)).start()
                    else:

                        @pl.when(core != home[axis])
                        def _():
                            remote(src, dst, gr_s.at[axis], gr_r.at[0], (partner, my)).start()

    def share(grad, part, got, send_sem, recv_sem):
        for k in (2, 1, 3):
            peer = (my + k) % n_mp
            part[k] = contract(grad, head[row_block(peer), :], 1, 1).astype(BF16)
            remote(part.at[k], got.at[k], send_sem, recv_sem, (me, peer)).start()
        return contract(grad, head[row_block(my), :], 1, 1)

    def gather_parts(own, got):
        for k in (1, 3, 2):
            own = own + got[k].astype(F32)
        return own

    phase("share_q")
    own_q = share(grad_q, part_q, got_q, pq_s, pq_r)

    phase("spread_q")
    spread(0, grad_q)
    phase("back_wait")
    await_got(returned.at[pl.ds(0, n_dp - 1)], ba_r)
    phase("grad_d")
    doc_back = jnp.dot(pick, returned[...].reshape(slots, cols), preferred_element_type=F32)
    grad_d = (pos_cols * qp.astype(F32) + doc_back).astype(BF16)
    spread(1, grad_d)
    phase("share_d")
    own_d = share(grad_d, part_d, got_d, pd_s, pd_r)
    phase("rt_wait")
    await_got(rt_others, rt_r)
    phase(None)

    def head_part(axis):
        with jax.named_scope("gather_h"):
            chip = 2 * slots
            await_got(grads[axis].at[pl.ds(0, slots)], gr_r.at[0])
            own_h[axis][...] = jnp.dot(
                rt_buf[:, :, :, :chip].reshape(n_mp * 2 * hrows, chip), grads[axis][:chip],
                preferred_element_type=F32,
            ).reshape(n_mp, 2 * hrows, -1)
            await_got(grads[axis].at[pl.ds(0, 6 * slots)], gr_r.at[1])
        for n in (2, 1, 3, 0):
            pos = (spots[axis] + n) % n_mp
            with jax.named_scope("head%d" % n):
                block = own_h[axis][pos] + jnp.dot(
                    rt_buf[pos, :, :, chip:].reshape(2 * hrows, 3 * chip), grads[axis][chip:],
                    preferred_element_type=F32,
                )
                part_h[axis][pl.ds(pos * 2, 2)] = block.astype(BF16).reshape(2, hrows, -1)
                if n == 0:
                    full_h[axis][...] = block[home[axis] * hrows : (home[axis] + 1) * hrows]
                    remote(
                        part_h[axis].at[pos * 2 + 1 - home[axis]], got_h[axis].at[0],
                        hg_s.at[axis], hg_r.at[axis], (partner, my),
                    ).start()
                for i in range(2 if n else 0):
                    remote(
                        part_h[axis].at[pos * 2 + i], got_h[axis].at[n],
                        hg_s.at[axis], hg_r.at[axis], (reducer(axis, pos, i), my),
                    ).start()

    for axis in range(2):
        pl.when(core == home[axis])(functools.partial(head_part, axis))
    phase("query_out")
    await_got(got_q.at[pl.ds(1, n_mp - 1)], pq_r)
    qg_ref[...] = gather_parts(own_q, got_q).astype(BF16)

    phase("doc_out")
    await_got(got_d.at[pl.ds(1, n_mp - 1)], pd_r)
    dg_ref[...] = gather_parts(own_d, got_d).astype(BF16)
    phase("head_out")
    for axis in range(2):
        columns = slice(cuts[axis], cuts[axis + 1])

        @pl.when(core == home[axis])
        def _():
            await_got(got_h[axis].at[pl.ds(1, n_mp - 1)], hg_r.at[axis])
            hg_ref[:, columns] = gather_parts(full_h[axis][...], got_h[axis])

        @pl.when(core != home[axis])
        def _():
            await_got(got_h[axis], hg_r.at[axis])
            hg_ref[:, columns] = gather_parts(got_h[axis][0].astype(F32), got_h[axis])

    phase("drain")
    await_sent(rows.at[pl.ds(0, 3)], ag_s)
    await_sent(out_buf.at[pl.ds(0, n_dp - 1)], fe_s)
    await_sent(rt_others, rt_s)
    await_sent(score_buf.at[pl.ds(0, n_mp - 1)], sc_s)
    await_sent(back_buf.at[pl.ds(0, n_dp - 1)], ba_s)
    for axis in range(2):

        @pl.when(core == home[axis])
        def _():
            await_sent(grads[axis].at[pl.ds(0, 6 * ql)], gr_s.at[axis])
            await_sent(part_h[axis].at[pl.ds(0, 7)], hg_s.at[axis])

        @pl.when(core != home[axis])
        def _():
            await_sent(grads[axis].at[pl.ds(0, 8 * ql)], gr_s.at[axis])

    await_sent(part_q.at[pl.ds(1, n_mp - 1)], pq_s)
    await_sent(part_d.at[pl.ds(1, n_mp - 1)], pd_s)
    phase(None)


def hand_out(a, b, c, out_a, out_b, out_c, sem):
    copies = [
        pltpu.make_async_copy(src, dst, sem.at[i])
        for i, (src, dst) in enumerate(((c, out_c), (a, out_a), (b, out_b)))
    ]
    for copy in copies:
        copy.start()
    for copy in copies:
        copy.wait()


def on_device(query_rows, doc_rows, head, logit_scale, loss_grad, shortlist, send_rows):
    ql, cols = query_rows.shape
    dma = pltpu.SemaphoreType.DMA
    one = dma(())
    hbm = pl.BlockSpec(memory_space=pltpu.HBM)
    vmem = pl.BlockSpec(memory_space=pltpu.VMEM)
    operands = (logit_scale, loss_grad.T, shortlist, send_rows, query_rows, doc_rows, head)
    shapes = (
        jax.ShapeDtypeStruct((ql, cols), BF16),
        jax.ShapeDtypeStruct((ql, cols), BF16),
        jax.ShapeDtypeStruct((80, cols), F32),
    )
    results = pl.pallas_call(
        kernel,
        out_shape=shapes,
        in_specs=[hbm] * 7,
        out_specs=(vmem, vmem, vmem),
        scratch_shapes=[
            pltpu.SMEM((NW,), F32),
            pltpu.VMEM((NW, ql), F32),
            pltpu.VMEM((ql, 128), jnp.int32),
            pltpu.VMEM((1, 128), jnp.int32),
            pltpu.VMEM((4, 2 * ql, cols), BF16),
            pltpu.VMEM((4 * cols, cols), BF16),
            pltpu.VMEM((4, 4, 2, 80, 128), BF16),
            pltpu.VMEM((4, 2, 80, 1024), BF16),
            pltpu.VMEM((1024, 384), BF16),
            pltpu.VMEM((1024, 256), BF16),
            pltpu.VMEM((32, 4, cols), BF16),
            pltpu.VMEM((32, 4, cols), BF16),
            pltpu.VMEM((32, 4, cols), BF16),
            pltpu.VMEM((32, 4, cols), BF16),
            pltpu.VMEM((4, ql + 8, 128), F32),
            pltpu.VMEM((4, ql, cols), BF16),
            pltpu.VMEM((4, ql, cols), BF16),
            pltpu.VMEM((4, ql, cols), BF16),
            pltpu.VMEM((4, ql, cols), BF16),
            pltpu.VMEM((4, 160, 384), F32),
            pltpu.VMEM((4, 160, 256), F32),
            pltpu.VMEM((80, 384), F32),
            pltpu.VMEM((80, 256), F32),
            pltpu.VMEM((8, 80, 384), BF16),
            pltpu.VMEM((8, 80, 256), BF16),
            pltpu.VMEM((4, 80, 384), BF16),
            pltpu.VMEM((4, 80, 256), BF16),
            dma((10,)), one, dma((10,)), one, one, one, one, one, one, one, one,
            dma((2,)), dma((2,)), one, one, one, one, dma((2,)), dma((2,)),
            pltpu.SemaphoreType.REGULAR((4,)),
        ],
        compiler_params=pltpu.CompilerParams(
            collective_id=0, has_side_effects=True, vmem_limit_bytes=48 * 1024 * 1024
        ),
    )(*[pltpu.with_memory_space_constraint(a, pltpu.HBM) for a in operands])
    anywhere = pl.BlockSpec(memory_space=pl.ANY)
    return pl.pallas_call(
        hand_out,
        out_shape=shapes,
        in_specs=[anywhere] * 3,
        out_specs=(anywhere,) * 3,
        scratch_shapes=[dma((3,))],
        compiler_params=pltpu.CompilerParams(vmem_limit_bytes=1024 * 1024),
    )(*results)


def solution(mesh):
    placed = (
        P("dp", "mp"),
        P("dp", "mp"),
        P(None, "mp"),
        P(),
        P("dp", None),
        P("dp", None),
        P("dp", None),
    )
    return jax.shard_map(
        on_device,
        mesh=mesh,
        in_specs=placed,
        out_specs=(P("dp", "mp"), P("dp", "mp"), P("dp", "mp")),
        check_vma=False,
    )
```
